32 devices in a mesh: dp: 1 (over z), row: 4 (over y), col: 8 (over x, core).
Axes of the slice: x: 4, y: 4, z: 1, core: 2. Of those that a mesh axis runs over, the one named last changes fastest.
The devices are a block of a 4x4x8 slice.
Arguments:
- x: bfloat16 [32768, 256], P(('dp', 'row', 'col'))
- route_idx: int32 [32768, 8], P(('dp', 'row', 'col'))
- gates: float32 [32768, 8], P(('dp', 'row', 'col'))
- w1: bfloat16 [64, 256, 128], P(('row', 'col'))
- w3: bfloat16 [64, 256, 128], P(('row', 'col'))
- w2: bfloat16 [64, 128, 256], P(('row', 'col'))
- dy: bfloat16 [32768, 256], P(('dp', 'row', 'col'))
Outputs:
- output 1: bfloat16 [32768, 256], P(('dp', 'row', 'col'))
- output 2: bfloat16 [32768, 256], P(('dp', 'row', 'col'))
- output 3: float32 [32768, 8], P(('dp', 'row', 'col'))
- output 4: float32 [64, 256, 128], P(('dp', 'row', 'col'))
- output 5: float32 [64, 256, 128], P(('dp', 'row', 'col'))
- output 6: float32 [64, 128, 256], P(('dp', 'row', 'col'))
All inputs are finite; a program needn't handle non-finite values.
Results may differ from the reference program's by a relative error of at most 0.001.
Values are sent between devices in bfloat16 or wider.
A program may use at most 768 MiB of HBM per device.

```python
import jax
import jax.numpy as jnp
from jax import lax

TOK = 1024
NDEV = 32
D = 256
FF = 128
EXPERTS = 64
TOP = 8

TG = NDEV * TOK
CAP = (4 * TOK * TOP + EXPERTS - 1) // EXPERTS
CG = NDEV * CAP
NH = max(1, min(TOP // 2, (8 * TOP) // NDEV))
HOT = 2 * EXPERTS // NDEV
NCOLD = EXPERTS - HOT


def setup_inputs(seed: int = 0, part: int = 0) -> dict:
    kw = jax.random.split(jax.random.key(seed), 3)
    kp = jax.random.split(jax.random.fold_in(jax.random.key(seed + 1), part), 8)
    w1 = (jax.random.normal(kw[0], (EXPERTS, D, FF), jnp.float32) * D ** -0.5).astype(jnp.bfloat16)
    w3 = (jax.random.normal(kw[1], (EXPERTS, D, FF), jnp.float32) * D ** -0.5).astype(jnp.bfloat16)
    w2 = (jax.random.normal(kw[2], (EXPERTS, FF, D), jnp.float32) * FF ** -0.5).astype(jnp.bfloat16)
    dmax = min(NH, HOT - NH, TOP - NH)
    sh = jax.random.randint(kp[2], (), 0, HOT)
    sc = jax.random.randint(kp[3], (), 0, NCOLD)
    dd = jax.random.randint(kp[0], (NDEV, TOK // 2), 0, dmax + 1)
    nh = jnp.stack([NH + dd, NH - dd], axis=-1).reshape(NDEV, TOK)
    nc = TOP - nh
    sth = jnp.cumsum(nh, axis=1) - nh
    stc = jnp.cumsum(nc, axis=1) - nc
    dev = jnp.arange(NDEV)[:, None, None]
    j = jnp.arange(TOP)[None, None, :]
    hot_ids = (sh + dev * (TOK * NH) + sth[:, :, None] + j) % HOT
    cold_ids = HOT + (sc + dev * (TOK * (TOP - NH)) + stc[:, :, None] + j - nh[:, :, None]) % NCOLD
    ids = jnp.where(j < nh[:, :, None], hot_ids, cold_ids).reshape(TG, TOP)
    ids = jax.random.permutation(kp[4], ids, axis=1, independent=True).astype(jnp.int32)
    gu = jax.random.uniform(kp[5], (TG, TOP), jnp.float32, 0.5, 1.5)
    gates = gu / jnp.sum(gu, axis=1, keepdims=True)
    x = jax.random.normal(kp[6], (TG, D), jnp.float32).astype(jnp.bfloat16)
    dy = jax.random.normal(kp[7], (TG, D), jnp.float32).astype(jnp.bfloat16)
    return {'x': x, 'route_idx': ids, 'gates': gates, 'w1': w1, 'w3': w3, 'w2': w2, 'dy': dy}


def reference(x, route_idx, gates, w1, w3, w2, dy):
    n = TG * TOP
    ef = route_idx.reshape(n)
    order = jnp.argsort(ef, stable=True).astype(jnp.int32)
    es = ef[order]
    first = jnp.searchsorted(es, es, side='left').astype(jnp.int32)
    rank = jnp.arange(n, dtype=jnp.int32) - first
    tab = jnp.full((EXPERTS, CG), n, jnp.int32).at[es, rank].set(order)
    gf = gates.reshape(n)

    def body(carry, inp):
        y_acc, dx_acc, dg = carry
        te, a1, a3, a2 = inp
        valid = te < n
        ai = jnp.minimum(te, n - 1)
        tk = ai // TOP
        xr = x[tk]
        xs = jnp.where(valid[:, None], xr, jnp.zeros_like(xr))
        u = jnp.dot(xs, a1, preferred_element_type=jnp.float32).astype(jnp.bfloat16).astype(jnp.float32)
        v = jnp.dot(xs, a3, preferred_element_type=jnp.float32).astype(jnp.bfloat16).astype(jnp.float32)
        sg = jax.nn.sigmoid(u)
        a = (u * sg * v).astype(jnp.bfloat16)
        o = jnp.dot(a, a2, preferred_element_type=jnp.float32).astype(jnp.bfloat16).astype(jnp.float32)
        g = jnp.where(valid, gf[ai], 0.0)
        y_acc = y_acc.at[tk].add(g[:, None] * o)
        dys = dy[tk].astype(jnp.float32)
        dg = dg.at[ai].add(jnp.where(valid, jnp.sum(dys * o, axis=1), 0.0))
        do = (g[:, None] * dys).astype(jnp.bfloat16)
        gw2 = jnp.dot(a.T, do, preferred_element_type=jnp.float32)
        da = jnp.dot(do, a2.T, preferred_element_type=jnp.float32)
        du = (da * v * sg * (1.0 + u * (1.0 - sg))).astype(jnp.bfloat16)
        dv = (da * u * sg).astype(jnp.bfloat16)
        gw1 = jnp.dot(xs.T, du, preferred_element_type=jnp.float32)
        gw3 = jnp.dot(xs.T, dv, preferred_element_type=jnp.float32)
        dxs = jnp.dot(du, a1.T, preferred_element_type=jnp.float32) + jnp.dot(dv, a3.T, preferred_element_type=jnp.float32)
        dx_acc = dx_acc.at[tk].add(dxs.astype(jnp.bfloat16).astype(jnp.float32))
        return (y_acc, dx_acc, dg), (gw1, gw3, gw2)

    init = (jnp.zeros((TG, D), jnp.float32), jnp.zeros((TG, D), jnp.float32), jnp.zeros((n,), jnp.float32))
    (y_acc, dx_acc, dg), (gw1, gw3, gw2) = lax.scan(body, init, (tab, w1, w3, w2))
    return (y_acc.astype(jnp.bfloat16), dx_acc.astype(jnp.bfloat16), dg.reshape(TG, TOP), gw1, gw3, gw2)
```

```python
import functools

import jax
import jax.numpy as jnp
from jax import lax
from jax.experimental import pallas as pl
from jax.experimental.pallas import tpu as pltpu
from jax.sharding import PartitionSpec as P

RINGS = 4
SLOTS = 6
LAG = 2
MESH = pl.DeviceIdType.MESH
F32 = jnp.float32
BF16 = jnp.bfloat16


def dot(a, b):
    return jnp.dot(a, b, preferred_element_type=F32)


def tdot(a, b):
    return lax.dot_general(a, b, (((0,), (0,)), ((), ())), preferred_element_type=F32)


def neighbours(k):
    dp = lax.axis_index('dp')
    row = lax.axis_index('row')
    col = lax.axis_index('col')
    x = col // 2
    c = col % 2
    s = (row + x) % k
    last = (s + 1) // k
    first = 1 - (s + k - 1) // k
    b = 1 - c

    def at(r, q, core):
        return (dp, r % k, (q % k) * 2 + core)

    n1 = at(row + c * last, x + c * (1 - last), b)
    p1 = at(row + k - b * first, x + k - b * (1 - first), b)
    n2 = at(row + c * (1 - last), x + c * last, b)
    p2 = at(row + k - b * (1 - first), x + k - b * first, b)
    return (n1, p1), (n2, p2)


def pick(i, a, b):
    return tuple((1 - i) * p + i * q for p, q in zip(a, b))


def kernel(n, k, x_hbm, dy_hbm, g_hbm, w1_ref, w3_ref, w2_ref, w2t_ref, w13t_ref,
           y_ref, dx_ref, dg_ref, gw1_ref, gw3_ref, gw2_ref,
           xs, gs, acc, own, part, gw13, load_sem, xsend, xrecv, gsend, grecv,
           asend, arecv, xfree, afree):
    t = xs.shape[2] // 2
    d = x_hbm.shape[1]
    el, ff, _ = w2_ref.shape
    top = g_hbm.shape[0] // 2
    h1, h2 = neighbours(k)
    first_expert = (lax.axis_index('row') * lax.axis_size('col') + lax.axis_index('col')) * el

    loads = []
    for r in range(RINGS):
        rows = pl.ds(r * t, t)
        loads.append(pltpu.make_async_copy(x_hbm.at[rows], xs.at[r, 0, pl.ds(0, t)], load_sem.at[r, 0]))
        loads.append(pltpu.make_async_copy(dy_hbm.at[rows], xs.at[r, 0, pl.ds(t, t)], load_sem.at[r, 1]))
        loads.append(pltpu.make_async_copy(g_hbm.at[:, rows], gs.at[r, 0], load_sem.at[r, 2]))
    for cp in loads:
        cp.start()

    barrier = pltpu.get_barrier_semaphore()
    for dev in (*h1, *h2):
        pl.semaphore_signal(barrier, inc=1, device_id=dev, device_id_type=MESH)

    gw13[...] = jnp.zeros_like(gw13)
    gw2_ref[...] = jnp.zeros_like(gw2_ref)
    for cp in loads:
        cp.wait()
    pl.semaphore_wait(barrier, 4)

    def tile(r, slot):
        x = xs[r, slot, 0:t, :]
        dy = xs[r, slot, t:2 * t, :]
        gates = gs[r, slot, 0:top, :]
        ids = gs[r, slot, top:2 * top, :]
        hit = [ids == (first_expert + e).astype(F32) for e in range(el)]
        sub = lax.broadcasted_iota(jnp.int32, gates.shape, 0)
        rows = jnp.zeros_like(gates)
        for e in range(el):
            ge = jnp.sum(jnp.where(hit[e], gates, 0.0), axis=0, keepdims=True)
            me = jnp.max(jnp.where(hit[e], 1.0, 0.0), axis=0, keepdims=True)
            rows = jnp.where(sub == e, ge, jnp.where(sub == el + e, me, rows))
        colm = rows.T
        dyf = dy.astype(F32)
        ua = dot(x, w1_ref[...])
        va = dot(x, w3_ref[...])
        y = None
        dx = None
        dgc = jnp.zeros((t, 128), F32)
        lane = lax.broadcasted_iota(jnp.int32, dgc.shape, 1)
        dudv = []
        for e in range(el):
            g = colm[:, e:e + 1]
            m = colm[:, el + e:el + e + 1] > 0.5
            u = jnp.where(m, ua[:, e * ff:(e + 1) * ff].astype(BF16).astype(F32), 0.0)
            v = jnp.where(m, va[:, e * ff:(e + 1) * ff].astype(BF16).astype(F32), 0.0)
            s = jax.nn.sigmoid(u)
            us = u * s
            a = (us * v).astype(BF16)
            o = dot(a, w2_ref[e]).astype(BF16).astype(F32)
            yo = g * o
            y = yo if y is None else y + yo
            dgc = jnp.where(lane == e, jnp.sum(dyf * o, axis=1, keepdims=True), dgc)
            do = (g * dyf).astype(BF16)
            gw2_ref[e] += tdot(a, do)
            da = dot(do, w2t_ref[e])
            du = (da * v * s * (1.0 + u * (1.0 - s))).astype(BF16)
            dv = (da * us).astype(BF16)
            dd = jnp.concatenate([du, dv], axis=1)
            dudv.append(dd)
            de = dot(dd, w13t_ref[e]).astype(BF16).astype(F32)
            dx = de if dx is None else dx + de
        gw13[...] += tdot(x, jnp.concatenate(dudv, axis=1))
        part[0:t, :] = y
        part[t:2 * t, :] = dx
        dgr = dgc.T
        dg = jnp.zeros_like(gates)
        for e in range(el):
            dg = jnp.where(hit[e], dgr[e:e + 1, :], dg)
        part[2 * t:2 * t + top, :] = dg

    def step(i, carry):
        st = i // RINGS
        r = i % RINGS
        cyc = r // 2
        back = r % 2
        fwd = pick(cyc, h1[0], h2[0])
        bwd = pick(cyc, h1[1], h2[1])
        nxt = pick(back, fwd, bwd)
        prv = pick(back, bwd, fwd)
        slot = st % SLOTS
        into = (st + 1) % SLOTS

        def xcopy(a, b):
            return pltpu.make_async_remote_copy(
                src_ref=xs.at[r, a], dst_ref=xs.at[r, b], send_sem=xsend.at[r, a], recv_sem=xrecv.at[r, b],
                device_id=nxt, device_id_type=MESH)

        def gcopy(a, b):
            return pltpu.make_async_remote_copy(
                src_ref=gs.at[r, a], dst_ref=gs.at[r, b], send_sem=gsend.at[r, a], recv_sem=grecv.at[r, b],
                device_id=nxt, device_id_type=MESH)

        def acopy(a, b):
            return pltpu.make_async_remote_copy(
                src_ref=acc.at[r, a], dst_ref=acc.at[r, b], send_sem=asend.at[r, a], recv_sem=arecv.at[r, b],
                device_id=nxt, device_id_type=MESH)

        done = st - LAG
        dslot = (st + SLOTS - LAG) % SLOTS

        @pl.when((done >= 0) & (done <= n - 2))
        def _():
            xcopy(dslot, dslot).wait_send()
            gcopy(dslot, dslot).wait_send()

        @pl.when((done >= 0) & (done <= n - 1 - SLOTS))
        def _():
            pl.semaphore_signal(xfree.at[r], inc=1, device_id=prv, device_id_type=MESH)

        @pl.when((done >= 1) & (done <= n - 1))
        def _():
            acopy(dslot, dslot).wait_send()

        @pl.when((done >= 1) & (done <= n - SLOTS))
        def _():
            pl.semaphore_signal(afree.at[r], inc=1, device_id=prv, device_id_type=MESH)

        @pl.when(st <= n - 1)
        def _():
            @pl.when(st >= 1)
            def _():
                gcopy(slot, slot).wait_recv()
                xcopy(slot, slot).wait_recv()

            @pl.when(st <= n - 2)
            def _():
                @pl.when(st + 1 >= SLOTS)
                def _():
                    pl.semaphore_wait(xfree.at[r], 1)

                gcopy(slot, into).start()
                xcopy(slot, into).start()

            tile(r, slot)

            @pl.when(st == 0)
            def _():
                own[r] = part[...]

            @pl.when(st == 1)
            def _():
                acc[r, slot] = part[...]

            @pl.when(st >= 2)
            def _():
                acopy(slot, slot).wait_recv()
                acc[r, slot] += part[...]

            @pl.when(st >= 1)
            def _():
                @pl.when(st >= SLOTS)
                def _():
                    pl.semaphore_wait(afree.at[r], 1)

                acopy(slot, into).start()

        @pl.when(st == n)
        def _():
            acopy(slot, slot).wait_recv()
            total = acc[r, slot] + own[r]
            rows = pl.ds(pl.multiple_of(r * t, t), t)
            y_ref[rows, :] = total[0:t].astype(BF16)
            dx_ref[rows, :] = total[t:2 * t].astype(BF16)
            dg_ref[r] = total[2 * t:2 * t + top]

        return carry

    lax.fori_loop(0, (n + 2) * RINGS, step, 0)

    for e in range(el):
        gw1_ref[e] = gw13[:, 2 * e * ff:(2 * e + 1) * ff]
        gw3_ref[e] = gw13[:, (2 * e + 1) * ff:(2 * e + 2) * ff]


def solution(mesh):
    k = mesh.shape['row']
    n = k * mesh.shape['col']
    grp = ('row', 'col')
    tspec = P(('dp', 'row', 'col'), None)
    wspec = P(grp, None, None)
    gspec = P(('dp', 'row', 'col'), None, None)

    def local(x, ridx, gates, w1, w3, w2, dy):
        tok, d = x.shape
        top = ridx.shape[1]
        el, ff, _ = w2.shape
        t = tok // RINGS
        g = jnp.concatenate([gates.T, ridx.T.astype(F32)], axis=0)
        w1c = jnp.concatenate([w1[e] for e in range(el)], axis=1)
        w3c = jnp.concatenate([w3[e] for e in range(el)], axis=1)
        w2t = w2.transpose(0, 2, 1)
        w13t = jnp.concatenate([w1.transpose(0, 2, 1), w3.transpose(0, 2, 1)], axis=1)
        rows = 2 * t + top
        vmem = pl.BlockSpec(memory_space=pltpu.VMEM)
        hbm = pl.BlockSpec(memory_space=pl.ANY)
        dma = pltpu.SemaphoreType.DMA((RINGS, SLOTS))
        flops = 2 * n * tok * el * 9 * d * ff
        y, dx, dg, gw1, gw3, gw2 = pl.pallas_call(
            functools.partial(kernel, n, k),
            out_shape=(
                jax.ShapeDtypeStruct((tok, d), BF16),
                jax.ShapeDtypeStruct((tok, d), BF16),
                jax.ShapeDtypeStruct((RINGS, top, t), F32),
                jax.ShapeDtypeStruct((el, d, ff), F32),
                jax.ShapeDtypeStruct((el, d, ff), F32),
                jax.ShapeDtypeStruct((el, ff, d), F32),
            ),
            in_specs=[hbm, hbm, hbm] + [vmem] * 5,
            out_specs=tuple([vmem] * 6),
            scratch_shapes=[
                pltpu.VMEM((RINGS, SLOTS, 2 * t, d), BF16),
                pltpu.VMEM((RINGS, SLOTS, 2 * top, t), F32),
                pltpu.VMEM((RINGS, SLOTS, rows, d), F32),
                pltpu.VMEM((RINGS, rows, d), F32),
                pltpu.VMEM((rows, d), F32),
                pltpu.VMEM((d, 2 * el * ff), F32),
                pltpu.SemaphoreType.DMA((RINGS, 3)),
                dma, dma, dma, dma, dma, dma,
                pltpu.SemaphoreType.REGULAR((RINGS,)),
                pltpu.SemaphoreType.REGULAR((RINGS,)),
            ],
            compiler_params=pltpu.CompilerParams(
                collective_id=0, has_side_effects=True, vmem_limit_bytes=56 * 1024 * 1024),
            cost_estimate=pl.CostEstimate(flops=flops, bytes_accessed=4 * tok * d * 2, transcendentals=n * tok * el * ff),
            name='moe_ring',
        )(x, dy, g, w1c, w3c, w2, w2t, w13t)
        return y, dx, dg.transpose(0, 2, 1).reshape(tok, top), gw1, gw3, gw2

    return jax.shard_map(local, mesh=mesh, in_specs=(tspec, tspec, tspec, wspec, wspec, wspec, tspec), out_specs=(tspec, tspec, tspec, gspec, gspec, gspec), check_vma=False)
```

```python
import functools

import jax
import jax.numpy as jnp
from jax import lax
from jax.experimental import pallas as pl
from jax.experimental.pallas import tpu as pltpu
from jax.sharding import PartitionSpec as P

RINGS = 4
SLOTS = 6
LAG = 2
MESH = pl.DeviceIdType.MESH
F32 = jnp.float32
BF16 = jnp.bfloat16


def dot(a, b):
    return jnp.dot(a, b, preferred_element_type=F32)


def tdot(a, b):
    return lax.dot_general(a, b, (((0,), (0,)), ((), ())), preferred_element_type=F32)


def neighbours(k):
    dp = lax.axis_index('dp')
    row = lax.axis_index('row')
    col = lax.axis_index('col')
    x = col // 2
    c = col % 2
    s = (row + x) % k
    last = (s + 1) // k
    first = 1 - (s + k - 1) // k
    b = 1 - c

    def at(r, q, core):
        return (dp, r % k, (q % k) * 2 + core)

    n1 = at(row + c * last, x + c * (1 - last), b)
    p1 = at(row + k - b * first, x + k - b * (1 - first), b)
    n2 = at(row + c * (1 - last), x + c * last, b)
    p2 = at(row + k - b * (1 - first), x + k - b * first, b)
    return (n1, p1), (n2, p2)


def pick(i, a, b):
    return tuple((1 - i) * p + i * q for p, q in zip(a, b))


def kernel(n, k, x_hbm, dy_hbm, g_hbm, w1_ref, w3_ref, w2_ref, w2t_ref, w13t_ref,
           y_ref, dx_ref, dg_ref, gw1_ref, gw3_ref, gw2_ref,
           xs, gs, acc, own, part, gw13, load_sem, xsend, xrecv, gsend, grecv,
           asend, arecv, xfree, afree):
    t = xs.shape[2] // 2
    d = x_hbm.shape[1]
    el, ff, _ = w2_ref.shape
    top = g_hbm.shape[0] // 2
    h1, h2 = neighbours(k)
    core = lax.axis_index('col') % 2
    first_expert = (lax.axis_index('row') * lax.axis_size('col') + lax.axis_index('col')) * el

    loads = []
    for r in range(RINGS):
        rows = pl.ds(r * t, t)
        loads.append(pltpu.make_async_copy(x_hbm.at[rows], xs.at[r, 0, pl.ds(0, t)], load_sem.at[r, 0]))
        loads.append(pltpu.make_async_copy(dy_hbm.at[rows], xs.at[r, 0, pl.ds(t, t)], load_sem.at[r, 1]))
        loads.append(pltpu.make_async_copy(g_hbm.at[:, rows], gs.at[r, 0], load_sem.at[r, 2]))
    for cp in loads:
        cp.start()

    barrier = pltpu.get_barrier_semaphore()
    for dev in (*h1, *h2):
        pl.semaphore_signal(barrier, inc=1, device_id=dev, device_id_type=MESH)

    gw13[...] = jnp.zeros_like(gw13)
    gw2_ref[...] = jnp.zeros_like(gw2_ref)
    for cp in loads:
        cp.wait()
    pl.semaphore_wait(barrier, 4)

    def tile(r, slot):
        x = xs[r, slot, 0:t, :]
        dy = xs[r, slot, t:2 * t, :]
        gates = gs[r, slot, 0:top, :]
        ids = gs[r, slot, top:2 * top, :]
        hit = [ids == (first_expert + e).astype(F32) for e in range(el)]
        sub = lax.broadcasted_iota(jnp.int32, gates.shape, 0)
        rows = jnp.zeros_like(gates)
        for e in range(el):
            ge = jnp.sum(jnp.where(hit[e], gates, 0.0), axis=0, keepdims=True)
            me = jnp.max(jnp.where(hit[e], 1.0, 0.0), axis=0, keepdims=True)
            rows = jnp.where(sub == e, ge, jnp.where(sub == el + e, me, rows))
        colm = rows.T
        dyf = dy.astype(F32)
        ua = dot(x, w1_ref[...])
        va = dot(x, w3_ref[...])
        y = None
        dx = None
        dgc = jnp.zeros((t, 128), F32)
        lane = lax.broadcasted_iota(jnp.int32, dgc.shape, 1)
        dudv = []
        for e in range(el):
            g = colm[:, e:e + 1]
            m = colm[:, el + e:el + e + 1] > 0.5
            u = jnp.where(m, ua[:, e * ff:(e + 1) * ff].astype(BF16).astype(F32), 0.0)
            v = jnp.where(m, va[:, e * ff:(e + 1) * ff].astype(BF16).astype(F32), 0.0)
            s = jax.nn.sigmoid(u)
            us = u * s
            a = (us * v).astype(BF16)
            o = dot(a, w2_ref[e]).astype(BF16).astype(F32)
            yo = g * o
            y = yo if y is None else y + yo
            dgc = jnp.where(lane == e, jnp.sum(dyf * o, axis=1, keepdims=True), dgc)
            do = (g * dyf).astype(BF16)
            gw2_ref[e] += tdot(a, do)
            da = dot(do, w2t_ref[e])
            du = (da * v * s * (1.0 + u * (1.0 - s))).astype(BF16)
            dv = (da * us).astype(BF16)
            dd = jnp.concatenate([du, dv], axis=1)
            dudv.append(dd)
            de = dot(dd, w13t_ref[e]).astype(BF16).astype(F32)
            dx = de if dx is None else dx + de
        gw13[...] += tdot(x, jnp.concatenate(dudv, axis=1))
        part[0:t, :] = y
        part[t:2 * t, :] = dx
        dgr = dgc.T
        dg = jnp.zeros_like(gates)
        for e in range(el):
            dg = jnp.where(hit[e], dgr[e:e + 1, :], dg)
        part[2 * t:2 * t + top, :] = dg

    def step(i, carry):
        link = (i % RINGS) // 2
        st = i // RINGS - 1 + link
        cyc = i % 2
        back = core + link * (1 - 2 * core)
        r = 2 * cyc + back
        fwd = pick(cyc, h1[0], h2[0])
        bwd = pick(cyc, h1[1], h2[1])
        nxt = pick(back, fwd, bwd)
        prv = pick(back, bwd, fwd)
        slot = (st + SLOTS) % SLOTS
        into = (st + 1) % SLOTS
        xslot = slot + (SLOTS - slot) * ((1 - link) * ((st + 1) // n))

        def xcopy(a, b):
            return pltpu.make_async_remote_copy(
                src_ref=xs.at[r, a], dst_ref=xs.at[r, b], send_sem=xsend.at[r, a], recv_sem=xrecv.at[r, b],
                device_id=nxt, device_id_type=MESH)

        def gcopy(a, b):
            return pltpu.make_async_remote_copy(
                src_ref=gs.at[r, a], dst_ref=gs.at[r, b], send_sem=gsend.at[r, a], recv_sem=grecv.at[r, b],
                device_id=nxt, device_id_type=MESH)

        def acopy(a, b):
            return pltpu.make_async_remote_copy(
                src_ref=acc.at[r, a], dst_ref=acc.at[r, b], send_sem=asend.at[r, a], recv_sem=arecv.at[r, b],
                device_id=nxt, device_id_type=MESH)

        def xlast():
            return pltpu.make_async_remote_copy(
                src_ref=xs.at[r, 0], dst_ref=xs.at[r, SLOTS], send_sem=xsend.at[r, SLOTS], recv_sem=xrecv.at[r, SLOTS],
                device_id=prv, device_id_type=MESH)

        def glast():
            return pltpu.make_async_remote_copy(
                src_ref=gs.at[r, 0], dst_ref=gs.at[r, SLOTS], send_sem=gsend.at[r, SLOTS], recv_sem=grecv.at[r, SLOTS],
                device_id=prv, device_id_type=MESH)

        def afirst():
            return pltpu.make_async_remote_copy(
                src_ref=acc.at[r, 1], dst_ref=acc.at[r, SLOTS], send_sem=asend.at[r, 1], recv_sem=arecv.at[r, SLOTS],
                device_id=prv, device_id_type=MESH)

        done = st - LAG
        dslot = (st + 2 * SLOTS - LAG) % SLOTS

        @pl.when((done >= 0) & (done <= n - 2 - link))
        def _():
            xcopy(dslot, dslot).wait_send()
            gcopy(dslot, dslot).wait_send()

        @pl.when((done == 0) & (link == 1))
        def _():
            xlast().wait_send()
            glast().wait_send()

        @pl.when((done >= 0) & (done <= n - 2 - SLOTS + link))
        def _():
            pl.semaphore_signal(xfree.at[r], inc=1, device_id=prv, device_id_type=MESH)

        @pl.when((done >= 1) & (done <= n - 1))
        def _():
            acopy(dslot, dslot).wait_send()

        @pl.when((done >= 1) & (done <= n - SLOTS))
        def _():
            pl.semaphore_signal(afree.at[r], inc=1, device_id=prv, device_id_type=MESH)

        @pl.when((st >= 0) & (st <= n - 1))
        def _():
            @pl.when(st >= 1)
            def _():
                gcopy(xslot, xslot).wait_recv()
                xcopy(xslot, xslot).wait_recv()

            @pl.when(st <= n - 2 - link)
            def _():
                @pl.when(st + 1 >= SLOTS)
                def _():
                    pl.semaphore_wait(xfree.at[r], 1)

                gcopy(slot, into).start()
                xcopy(slot, into).start()

            @pl.when((st == 0) & (link == 1))
            def _():
                glast().start()
                xlast().start()

            tile(r, xslot)

            @pl.when(st == 0)
            def _():
                own[r] = part[...]

            @pl.when((st >= 1) & (st <= 2 - link))
            def _():
                acc[r, slot] = part[...]

            @pl.when(st >= 3 - link)
            def _():
                acopy(slot, slot).wait_recv()
                acc[r, slot] += part[...]

            @pl.when((st == 1) & (link == 1))
            def _():
                afirst().start()

            @pl.when(st >= 1 + link)
            def _():
                @pl.when(st >= SLOTS)
                def _():
                    pl.semaphore_wait(afree.at[r], 1)

                acopy(slot, into).start()

        @pl.when(st == n)
        def _():
            acopy(slot, slot).wait_recv()
            own[r] += acc[r, slot]

            @pl.when(link == 0)
            def _():
                acopy(SLOTS, SLOTS).wait_recv()
                own[r] += acc[r, SLOTS]

            total = own[r]
            rows = pl.ds(pl.multiple_of(r * t, t), t)
            y_ref[rows, :] = total[0:t].astype(BF16)
            dx_ref[rows, :] = total[t:2 * t].astype(BF16)
            dg_ref[r] = total[2 * t:2 * t + top]

        return carry

    lax.fori_loop(0, (n + LAG + 1) * RINGS, step, 0)

    for e in range(el):
        gw1_ref[e] = gw13[:, 2 * e * ff:(2 * e + 1) * ff]
        gw3_ref[e] = gw13[:, (2 * e + 1) * ff:(2 * e + 2) * ff]


def solution(mesh):
    k = mesh.shape['row']
    n = k * mesh.shape['col']
    grp = ('row', 'col')
    tspec = P(('dp', 'row', 'col'), None)
    wspec = P(grp, None, None)
    gspec = P(('dp', 'row', 'col'), None, None)

    def local(x, ridx, gates, w1, w3, w2, dy):
        tok, d = x.shape
        top = ridx.shape[1]
        el, ff, _ = w2.shape
        t = tok // RINGS
        g = jnp.concatenate([gates.T, ridx.T.astype(F32)], axis=0)
        w1c = jnp.concatenate([w1[e] for e in range(el)], axis=1)
        w3c = jnp.concatenate([w3[e] for e in range(el)], axis=1)
        w2t = w2.transpose(0, 2, 1)
        w13t = jnp.concatenate([w1.transpose(0, 2, 1), w3.transpose(0, 2, 1)], axis=1)
        rows = 2 * t + top
        vmem = pl.BlockSpec(memory_space=pltpu.VMEM)
        hbm = pl.BlockSpec(memory_space=pl.ANY)
        dma = pltpu.SemaphoreType.DMA((RINGS, SLOTS + 1))
        flops = 2 * n * tok * el * 9 * d * ff
        y, dx, dg, gw1, gw3, gw2 = pl.pallas_call(
            functools.partial(kernel, n, k),
            out_shape=(
                jax.ShapeDtypeStruct((tok, d), BF16),
                jax.ShapeDtypeStruct((tok, d), BF16),
                jax.ShapeDtypeStruct((RINGS, top, t), F32),
                jax.ShapeDtypeStruct((el, d, ff), F32),
                jax.ShapeDtypeStruct((el, d, ff), F32),
                jax.ShapeDtypeStruct((el, ff, d), F32),
            ),
            in_specs=[hbm, hbm, hbm] + [vmem] * 5,
            out_specs=tuple([vmem] * 6),
            scratch_shapes=[
                pltpu.VMEM((RINGS, SLOTS + 1, 2 * t, d), BF16),
                pltpu.VMEM((RINGS, SLOTS + 1, 2 * top, t), F32),
                pltpu.VMEM((RINGS, SLOTS + 1, rows, d), F32),
                pltpu.VMEM((RINGS, rows, d), F32),
                pltpu.VMEM((rows, d), F32),
                pltpu.VMEM((d, 2 * el * ff), F32),
                pltpu.SemaphoreType.DMA((RINGS, 3)),
                dma, dma, dma, dma, dma, dma,
                pltpu.SemaphoreType.REGULAR((RINGS,)),
                pltpu.SemaphoreType.REGULAR((RINGS,)),
            ],
            compiler_params=pltpu.CompilerParams(
                collective_id=0, has_side_effects=True, vmem_limit_bytes=56 * 1024 * 1024),
            cost_estimate=pl.CostEstimate(flops=flops, bytes_accessed=4 * tok * d * 2, transcendentals=n * tok * el * ff),
            name='moe_ring',
        )(x, dy, g, w1c, w3c, w2, w2t, w13t)
        return y, dx, dg.transpose(0, 2, 1).reshape(tok, top), gw1, gw3, gw2

    return jax.shard_map(local, mesh=mesh, in_specs=(tspec, tspec, tspec, wspec, wspec, wspec, tspec), out_specs=(tspec, tspec, tspec, gspec, gspec, gspec), check_vma=False)
```

```python
import functools

import jax
import jax.numpy as jnp
from jax import lax
from jax.experimental import pallas as pl
from jax.experimental.pallas import tpu as pltpu
from jax.sharding import PartitionSpec as P

RINGS = 4
SLOTS = 6
LAG = 2
MESH = pl.DeviceIdType.MESH
F32 = jnp.float32
BF16 = jnp.bfloat16


def dot(a, b):
    return jnp.dot(a, b, preferred_element_type=F32)


def tdot(a, b):
    return lax.dot_general(a, b, (((0,), (0,)), ((), ())), preferred_element_type=F32)


def neighbours(k):
    dp = lax.axis_index('dp')
    row = lax.axis_index('row')
    col = lax.axis_index('col')
    x = col // 2
    c = col % 2
    s = (row + x) % k
    last = (s + 1) // k
    first = 1 - (s + k - 1) // k
    b = 1 - c

    def at(r, q, core):
        return (dp, r % k, (q % k) * 2 + core)

    n1 = at(row + c * last, x + c * (1 - last), b)
    p1 = at(row + k - b * first, x + k - b * (1 - first), b)
    n2 = at(row + c * (1 - last), x + c * last, b)
    p2 = at(row + k - b * (1 - first), x + k - b * first, b)
    return (n1, p1), (n2, p2)


def pick(i, a, b):
    return tuple((1 - i) * p + i * q for p, q in zip(a, b))


def kernel(n, k, x_hbm, dy_hbm, g_hbm, id_hbm, w1_hbm, w3_hbm, w2_hbm,
           y_ref, dx_ref, dg_ref, gw1_ref, gw3_ref, gw2_ref,
           xs, gs, acc, own, part, gw13, ids, w1_ref, w3_ref, w2_ref, w2t_ref, w13t_ref,
           load_sem, xsend, xrecv, gsend, grecv, asend, arecv, xfree, afree):
    t = gs.shape[3]
    d = x_hbm.shape[1]
    el, ff, _ = w2_hbm.shape
    top = g_hbm.shape[0]
    h1, h2 = neighbours(k)
    core = lax.axis_index('col') % 2
    first_expert = (lax.axis_index('row') * lax.axis_size('col') + lax.axis_index('col')) * el

    def load(src, dst, i, j):
        cp = pltpu.make_async_copy(src, dst, load_sem.at[i, j])
        cp.start()
        return cp

    first = [load(id_hbm, ids, RINGS, 0)]
    for r in range(RINGS):
        rows = pl.ds(r * t, t)
        first.append(load(x_hbm.at[rows], xs.at[r, 0, pl.ds(0, t)], r, 0))
        first.append(load(dy_hbm.at[rows], xs.at[r, 0, pl.ds(t, t)], r, 1))
        first.append(load(g_hbm.at[:, rows], gs.at[r, 0], r, 2))
    later = [load(w2_hbm, w2_ref, RINGS, 1)]
    for e in range(el):
        cols = pl.ds(e * ff, ff)
        later.append(load(w1_hbm.at[e], w1_ref.at[:, cols], RINGS + 1, e))
        later.append(load(w3_hbm.at[e], w3_ref.at[:, cols], RINGS + 2, e))

    barrier = pltpu.get_barrier_semaphore()
    for dev in (*h1, *h2):
        pl.semaphore_signal(barrier, inc=1, device_id=dev, device_id_type=MESH)

    for cp in first:
        cp.wait()
    for r in range(RINGS):
        xs[r, 0, 2 * t:2 * t + top, :] = ids[:, r * t:(r + 1) * t].astype(F32).astype(BF16)
    gw13[...] = jnp.zeros_like(gw13)
    gw2_ref[...] = jnp.zeros_like(gw2_ref)
    pl.semaphore_wait(barrier, 4)

    def tile(r, slot):
        x = xs[r, slot, 0:t, :]
        dy = xs[r, slot, t:2 * t, :]
        gates = gs[r, slot, 0:top, :]
        dest = xs[r, slot, 2 * t:2 * t + top, :].astype(F32)
        hit = [dest == (first_expert + e).astype(F32) for e in range(el)]
        sub = lax.broadcasted_iota(jnp.int32, gates.shape, 0)
        rows = jnp.zeros_like(gates)
        for e in range(el):
            ge = jnp.sum(jnp.where(hit[e], gates, 0.0), axis=0, keepdims=True)
            me = jnp.max(jnp.where(hit[e], 1.0, 0.0), axis=0, keepdims=True)
            rows = jnp.where(sub == e, ge, jnp.where(sub == el + e, me, rows))
        colm = rows.T
        dyf = dy.astype(F32)
        ua = dot(x, w1_ref[...])
        va = dot(x, w3_ref[...])
        y = None
        dx = None
        dgc = jnp.zeros((t, 128), F32)
        lane = lax.broadcasted_iota(jnp.int32, dgc.shape, 1)
        dudv = []
        for e in range(el):
            g = colm[:, e:e + 1]
            m = colm[:, el + e:el + e + 1] > 0.5
            u = jnp.where(m, ua[:, e * ff:(e + 1) * ff].astype(BF16).astype(F32), 0.0)
            v = jnp.where(m, va[:, e * ff:(e + 1) * ff].astype(BF16).astype(F32), 0.0)
            s = jax.nn.sigmoid(u)
            us = u * s
            a = (us * v).astype(BF16)
            o = dot(a, w2_ref[e]).astype(BF16).astype(F32)
            yo = g * o
            y = yo if y is None else y + yo
            dgc = jnp.where(lane == e, jnp.sum(dyf * o, axis=1, keepdims=True), dgc)
            do = (g * dyf).astype(BF16)
            gw2_ref[e] += tdot(a, do)
            da = dot(do, w2t_ref[e])
            du = (da * v * s * (1.0 + u * (1.0 - s))).astype(BF16)
            dv = (da * us).astype(BF16)
            dd = jnp.concatenate([du, dv], axis=1)
            dudv.append(dd)
            de = dot(dd, w13t_ref[e]).astype(BF16).astype(F32)
            dx = de if dx is None else dx + de
        gw13[...] += tdot(x, jnp.concatenate(dudv, axis=1))
        part[0:t, :] = y
        part[t:2 * t, :] = dx
        dgr = dgc.T
        dg = jnp.zeros_like(gates)
        for e in range(el):
            dg = jnp.where(hit[e], dgr[e:e + 1, :], dg)
        part[2 * t:2 * t + top, :] = dg

    def ring(i):
        link = i // 2
        cyc = i % 2
        back = core + link * (1 - 2 * core)
        fwd = pick(cyc, h1[0], h2[0])
        bwd = pick(cyc, h1[1], h2[1])
        return link, 2 * cyc + back, pick(back, fwd, bwd), pick(back, bwd, fwd)

    def send(buf, sends, recvs, r, a, b, dev, s=None):
        return pltpu.make_async_remote_copy(
            src_ref=buf.at[r, a], dst_ref=buf.at[r, b], send_sem=sends.at[r, a if s is None else s],
            recv_sem=recvs.at[r, b], device_id=dev, device_id_type=MESH)

    def xcopies(r, a, b, dev, s=None):
        return send(gs, gsend, grecv, r, a, b, dev, s), send(xs, xsend, xrecv, r, a, b, dev, s)

    def begin(i, carry):
        link, r, nxt, prv = ring(RINGS - 1 - i)
        for cp in xcopies(r, 0, 1, nxt):
            cp.start()

        @pl.when(link == 1)
        def _():
            for cp in xcopies(r, 0, SLOTS, prv, SLOTS):
                cp.start()

        return carry

    lax.fori_loop(0, RINGS, begin, 0)

    for cp in later:
        cp.wait()
    for e in range(el):
        cols = slice(e * ff, (e + 1) * ff)
        w2t_ref[e] = w2_ref[e].astype(F32).T.astype(BF16)
        w13t_ref[e, 0:ff, :] = w1_ref[:, cols].astype(F32).T.astype(BF16)
        w13t_ref[e, ff:2 * ff, :] = w3_ref[:, cols].astype(F32).T.astype(BF16)

    def step(i, carry):
        link, r, nxt, prv = ring(i % RINGS)
        st = i // RINGS - 1 + link
        slot = (st + SLOTS) % SLOTS
        into = (st + 1) % SLOTS
        two = (st + 2) % SLOTS
        xslot = slot + (SLOTS - slot) * ((1 - link) * ((st + 1) // n))
        into_x = into + (SLOTS - into) * ((1 - link) * ((st + 2) // n))
        gone = (st + SLOTS - 1) % SLOTS
        done = st - LAG
        dslot = (st + 2 * SLOTS - LAG) % SLOTS

        def acopy(a, b):
            return send(acc, asend, arecv, r, a, b, nxt)

        @pl.when((st >= 1) & (st <= n - 1 - link))
        def _():
            for cp in xcopies(r, gone, gone, nxt):
                cp.wait_send()

        @pl.when((st == 1) & (link == 1))
        def _():
            for cp in xcopies(r, 0, SLOTS, prv, SLOTS):
                cp.wait_send()

        @pl.when((st >= 1) & (st <= n - 1 - SLOTS + link))
        def _():
            pl.semaphore_signal(xfree.at[r], inc=1, device_id=prv, device_id_type=MESH)

        @pl.when((done >= 1) & (done <= n - 1))
        def _():
            acopy(dslot, dslot).wait_send()

        @pl.when((done >= 1) & (done <= n - SLOTS))
        def _():
            pl.semaphore_signal(afree.at[r], inc=1, device_id=prv, device_id_type=MESH)

        @pl.when((st >= 0) & (st <= n - 1))
        def _():
            tile(r, xslot)

            @pl.when(st <= n - 2)
            def _():
                for cp in xcopies(r, into_x, into_x, nxt):
                    cp.wait_recv()

            @pl.when(st <= n - 3 - link)
            def _():
                @pl.when(st + 2 >= SLOTS)
                def _():
                    pl.semaphore_wait(xfree.at[r], 1)

                for cp in xcopies(r, into, two, nxt):
                    cp.start()

            @pl.when(st == 0)
            def _():
                own[r] = part[...]

            @pl.when((st >= 1) & (st <= 2 - link))
            def _():
                acc[r, slot] = part[...]

            @pl.when(st >= 3 - link)
            def _():
                acopy(slot, slot).wait_recv()
                acc[r, slot] += part[...]

            @pl.when((st == 1) & (link == 1))
            def _():
                send(acc, asend, arecv, r, 1, SLOTS, prv).start()

            @pl.when(st >= 1 + link)
            def _():
                @pl.when(st >= SLOTS)
                def _():
                    pl.semaphore_wait(afree.at[r], 1)

                acopy(slot, into).start()

        @pl.when(i == n * RINGS + 2)
        def _():
            for e in range(el):
                gw1_ref[e] = gw13[:, 2 * e * ff:(2 * e + 1) * ff]
                gw3_ref[e] = gw13[:, (2 * e + 1) * ff:(2 * e + 2) * ff]

        @pl.when((st == n - 1) & (link == 0))
        def _():
            acopy(SLOTS, SLOTS).wait_recv()
            own[r] += acc[r, SLOTS]

        @pl.when(st == n)
        def _():
            acopy(slot, slot).wait_recv()
            total = acc[r, slot] + own[r]
            rows = pl.ds(pl.multiple_of(r * t, t), t)
            y_ref[rows, :] = total[0:t].astype(BF16)
            dx_ref[rows, :] = total[t:2 * t].astype(BF16)
            dg_ref[r] = total[2 * t:2 * t + top]

        return carry

    lax.fori_loop(0, (n + LAG + 1) * RINGS, step, 0)


def solution(mesh):
    k = mesh.shape['row']
    n = k * mesh.shape['col']
    grp = ('row', 'col')
    tspec = P(('dp', 'row', 'col'), None)
    wspec = P(grp, None, None)
    gspec = P(('dp', 'row', 'col'), None, None)

    def local(x, ridx, gates, w1, w3, w2, dy):
        tok, d = x.shape
        top = ridx.shape[1]
        el, ff, _ = w2.shape
        t = tok // RINGS
        rows = 2 * t + top
        vmem = pl.BlockSpec(memory_space=pltpu.VMEM)
        hbm = pl.BlockSpec(memory_space=pltpu.HBM)
        dma = pltpu.SemaphoreType.DMA((RINGS, SLOTS + 1))
        flops = 2 * n * tok * el * 9 * d * ff
        y, dx, dg, gw1, gw3, gw2 = pl.pallas_call(
            functools.partial(kernel, n, k),
            out_shape=(
                jax.ShapeDtypeStruct((tok, d), BF16),
                jax.ShapeDtypeStruct((tok, d), BF16),
                jax.ShapeDtypeStruct((RINGS, top, t), F32),
                jax.ShapeDtypeStruct((el, d, ff), F32),
                jax.ShapeDtypeStruct((el, d, ff), F32),
                jax.ShapeDtypeStruct((el, ff, d), F32),
            ),
            in_specs=[hbm] * 7,
            out_specs=tuple([vmem] * 6),
            scratch_shapes=[
                pltpu.VMEM((RINGS, SLOTS + 1, rows, d), BF16),
                pltpu.VMEM((RINGS, SLOTS + 1, top, t), F32),
                pltpu.VMEM((RINGS, SLOTS + 1, rows, d), F32),
                pltpu.VMEM((RINGS, rows, d), F32),
                pltpu.VMEM((rows, d), F32),
                pltpu.VMEM((d, 2 * el * ff), F32),
                pltpu.VMEM((top, tok), jnp.int32),
                pltpu.VMEM((d, el * ff), BF16),
                pltpu.VMEM((d, el * ff), BF16),
                pltpu.VMEM((el, ff, d), BF16),
                pltpu.VMEM((el, d, ff), BF16),
                pltpu.VMEM((el, 2 * ff, d), BF16),
                pltpu.SemaphoreType.DMA((RINGS + 3, max(3, el))),
                dma, dma, dma, dma, dma, dma,
                pltpu.SemaphoreType.REGULAR((RINGS,)),
                pltpu.SemaphoreType.REGULAR((RINGS,)),
            ],
            compiler_params=pltpu.CompilerParams(
                collective_id=0, has_side_effects=True, vmem_limit_bytes=56 * 1024 * 1024),
            cost_estimate=pl.CostEstimate(flops=flops, bytes_accessed=4 * tok * d * 2, transcendentals=n * tok * el * ff),
            name='moe_ring',
        )(x, dy, gates.T, ridx.T, w1, w3, w2)
        return y, dx, dg.transpose(0, 2, 1).reshape(tok, top), gw1, gw3, gw2

    return jax.shard_map(local, mesh=mesh, in_specs=(tspec, tspec, tspec, wspec, wspec, wspec, tspec), out_specs=(tspec, tspec, tspec, gspec, gspec, gspec), check_vma=False)
```

```python
import functools

import jax
import jax.numpy as jnp
from jax import lax
from jax.experimental import pallas as pl
from jax.experimental.pallas import tpu as pltpu
from jax.sharding import PartitionSpec as P

RINGS = 4
SLOTS = 8
HOME = SLOTS + 1
LAG = 2
OWN_STEP = 5
MESH = pl.DeviceIdType.MESH
F32 = jnp.float32
BF16 = jnp.bfloat16


def dot(a, b):
    return jnp.dot(a, b, preferred_element_type=F32)


def tdot(a, b):
    return lax.dot_general(a, b, (((0,), (0,)), ((), ())), preferred_element_type=F32)


def neighbours(k):
    dp = lax.axis_index('dp')
    row = lax.axis_index('row')
    col = lax.axis_index('col')
    x = col // 2
    c = col % 2
    s = (row + x) % k
    last = (s + 1) // k
    first = 1 - (s + k - 1) // k
    b = 1 - c

    def at(r, q, core):
        return (dp, r % k, (q % k) * 2 + core)

    n1 = at(row + c * last, x + c * (1 - last), b)
    p1 = at(row + k - b * first, x + k - b * (1 - first), b)
    n2 = at(row + c * (1 - last), x + c * last, b)
    p2 = at(row + k - b * (1 - first), x + k - b * first, b)
    return (n1, p1), (n2, p2)


def pick(i, a, b):
    return tuple((1 - i) * p + i * q for p, q in zip(a, b))


def kernel(n, k, x_hbm, dy_hbm, g_hbm, id_hbm, w1_hbm, w3_hbm, w2_hbm,
           y_hbm, dx_hbm, dg_hbm, gw13_hbm, gw2_hbm,
           xs, gs, acc, own, part, gw13, gw2_ref, out, ids, w1_ref, w3_ref, w2_ref, w2t_ref, w13t_ref,
           load_sem, out_sem, xsend, xrecv, gsend, grecv, asend, arecv, xfree, afree):
    t = gs.shape[3]
    d = x_hbm.shape[1]
    el, ff, _ = w2_hbm.shape
    top = g_hbm.shape[0]
    h1, h2 = neighbours(k)
    core = lax.axis_index('col') % 2
    first_expert = (lax.axis_index('row') * lax.axis_size('col') + lax.axis_index('col')) * el

    def load(src, dst, i, j):
        cp = pltpu.make_async_copy(src, dst, load_sem.at[i, j])
        cp.start()
        return cp

    first = [load(id_hbm, ids, RINGS, 0)]
    for r in range(RINGS):
        rows = pl.ds(r * t, t)
        first.append(load(x_hbm.at[rows], xs.at[r, HOME, pl.ds(0, t)], r, 0))
        first.append(load(dy_hbm.at[rows], xs.at[r, HOME, pl.ds(t, t)], r, 1))
        first.append(load(g_hbm.at[:, rows], gs.at[r, HOME], r, 2))
    later = [load(w2_hbm, w2_ref, RINGS, 1)]
    for e in range(el):
        cols = pl.ds(e * ff, ff)
        later.append(load(w1_hbm.at[e], w1_ref.at[:, cols], RINGS + 1, e))
        later.append(load(w3_hbm.at[e], w3_ref.at[:, cols], RINGS + 2, e))

    barrier = pltpu.get_barrier_semaphore()
    for dev in (*h1, *h2):
        pl.semaphore_signal(barrier, inc=1, device_id=dev, device_id_type=MESH)

    for cp in first:
        cp.wait()
    for r in range(RINGS):
        xs[r, HOME, 2 * t:2 * t + top, :] = ids[:, r * t:(r + 1) * t].astype(F32).astype(BF16)
    gw13[...] = jnp.zeros_like(gw13)
    gw2_ref[...] = jnp.zeros_like(gw2_ref)
    pl.semaphore_wait(barrier, 4)

    def tile(r, slot):
        x = xs[r, slot, 0:t, :]
        dy = xs[r, slot, t:2 * t, :]
        gates = gs[r, slot, 0:top, :]
        dest = xs[r, slot, 2 * t:2 * t + top, :].astype(F32)
        hit = [dest == (first_expert + e).astype(F32) for e in range(el)]
        sub = lax.broadcasted_iota(jnp.int32, gates.shape, 0)
        rows = jnp.zeros_like(gates)
        for e in range(el):
            ge = jnp.sum(jnp.where(hit[e], gates, 0.0), axis=0, keepdims=True)
            me = jnp.max(jnp.where(hit[e], 1.0, 0.0), axis=0, keepdims=True)
            rows = jnp.where(sub == e, ge, jnp.where(sub == el + e, me, rows))
        colm = rows.T
        dyf = dy.astype(F32)
        ua = dot(x, w1_ref[...])
        va = dot(x, w3_ref[...])
        y = None
        dx = None
        dgc = jnp.zeros((t, 128), F32)
        lane = lax.broadcasted_iota(jnp.int32, dgc.shape, 1)
        dudv = []
        for e in range(el):
            g = colm[:, e:e + 1]
            m = colm[:, el + e:el + e + 1] > 0.5
            u = jnp.where(m, ua[:, e * ff:(e + 1) * ff].astype(BF16).astype(F32), 0.0)
            v = jnp.where(m, va[:, e * ff:(e + 1) * ff].astype(BF16).astype(F32), 0.0)
            s = jax.nn.sigmoid(u)
            us = u * s
            a = (us * v).astype(BF16)
            o = dot(a, w2_ref[e]).astype(BF16).astype(F32)
            yo = g * o
            y = yo if y is None else y + yo
            dgc = jnp.where(lane == e, jnp.sum(dyf * o, axis=1, keepdims=True), dgc)
            do = (g * dyf).astype(BF16)
            gw2_ref[e] += tdot(a, do)
            da = dot(do, w2t_ref[e])
            du = (da * v * s * (1.0 + u * (1.0 - s))).astype(BF16)
            dv = (da * us).astype(BF16)
            dd = jnp.concatenate([du, dv], axis=1)
            dudv.append(dd)
            de = dot(dd, w13t_ref[e]).astype(BF16).astype(F32)
            dx = de if dx is None else dx + de
        gw13[...] += tdot(x, jnp.concatenate(dudv, axis=1))
        part[0:t, :] = y
        part[t:2 * t, :] = dx
        dgr = dgc.T
        dg = jnp.zeros_like(gates)
        for e in range(el):
            dg = jnp.where(hit[e], dgr[e:e + 1, :], dg)
        part[2 * t:2 * t + top, :] = dg

    def ring(i):
        link = i // 2
        cyc = i % 2
        back = core + link * (1 - 2 * core)
        fwd = pick(cyc, h1[0], h2[0])
        bwd = pick(cyc, h1[1], h2[1])
        return link, 2 * cyc + back, pick(back, fwd, bwd), pick(back, bwd, fwd)

    def send(buf, sends, recvs, r, a, b, dev, s=None):
        return pltpu.make_async_remote_copy(
            src_ref=buf.at[r, a], dst_ref=buf.at[r, b], send_sem=sends.at[r, a if s is None else s],
            recv_sem=recvs.at[r, b], device_id=dev, device_id_type=MESH)

    def xcopies(r, a, b, dev, s=None):
        return send(gs, gsend, grecv, r, a, b, dev, s), send(xs, xsend, xrecv, r, a, b, dev, s)

    def begin(i, carry):
        link, r, nxt, prv = ring(RINGS - 1 - i)
        for cp in xcopies(r, HOME, 1, nxt):
            cp.start()

        @pl.when(link == 1)
        def _():
            for cp in xcopies(r, HOME, SLOTS, prv, SLOTS):
                cp.start()

        return carry

    lax.fori_loop(0, RINGS, begin, 0)

    for cp in later:
        cp.wait()
    for e in range(el):
        cols = slice(e * ff, (e + 1) * ff)
        w2t_ref[e] = w2_ref[e].astype(F32).T.astype(BF16)
        w13t_ref[e, 0:ff, :] = w1_ref[:, cols].astype(F32).T.astype(BF16)
        w13t_ref[e, ff:2 * ff, :] = w3_ref[:, cols].astype(F32).T.astype(BF16)

    def weight_grads():
        return (pltpu.make_async_copy(gw13, gw13_hbm, out_sem.at[RINGS, 0]),
                pltpu.make_async_copy(gw2_ref, gw2_hbm, out_sem.at[RINGS, 1]))

    def results(r):
        rows = pl.ds(pl.multiple_of(r * t, t), t)
        return (pltpu.make_async_copy(out.at[r, pl.ds(0, t)], y_hbm.at[rows], out_sem.at[r, 0]),
                pltpu.make_async_copy(out.at[r, pl.ds(t, t)], dx_hbm.at[rows], out_sem.at[r, 1]),
                pltpu.make_async_copy(own.at[r, pl.ds(2 * t, top)], dg_hbm.at[r], out_sem.at[r, 2]))

    def step(i, carry):
        link, r, nxt, prv = ring(i % RINGS)
        st = i // RINGS - 1 + link
        slot = (st + SLOTS) % SLOTS
        into = (st + 1) % SLOTS
        two = (st + 2) % SLOTS
        xslot = slot + (SLOTS - slot) * ((1 - link) * ((st + 1) // n))
        into_x = into + (SLOTS - into) * ((1 - link) * ((st + 2) // n))
        gone = (st + SLOTS - 1) % SLOTS
        done = st - LAG
        dslot = (st + 2 * SLOTS - LAG) % SLOTS

        def acopy(a, b):
            return send(acc, asend, arecv, r, a, b, nxt)

        @pl.when((st >= 2) & (st <= n - 1 - link))
        def _():
            for cp in xcopies(r, gone, gone, nxt):
                cp.wait_send()

        @pl.when(st == 2)
        def _():
            for cp in xcopies(r, HOME, HOME, nxt):
                cp.wait_send()

        @pl.when((st == 2) & (link == 1))
        def _():
            for cp in xcopies(r, HOME, SLOTS, prv, SLOTS):
                cp.wait_send()

        @pl.when((st >= 2) & (st <= n - 1 - SLOTS + link))
        def _():
            pl.semaphore_signal(xfree.at[r], inc=1, device_id=prv, device_id_type=MESH)

        @pl.when((done >= 1) & (done <= n - 1))
        def _():
            acopy(dslot, dslot).wait_send()

        @pl.when((done >= 1) & (done <= n - SLOTS))
        def _():
            pl.semaphore_signal(afree.at[r], inc=1, device_id=prv, device_id_type=MESH)

        @pl.when((st >= 0) & (st <= n - 1))
        def _():
            @pl.when(st >= 1)
            def _():
                tile(r, xslot)

            @pl.when(st <= n - 2)
            def _():
                for cp in xcopies(r, into_x, into_x, nxt):
                    cp.wait_recv()

            @pl.when(st <= n - 3 - link)
            def _():
                @pl.when(st + 2 > SLOTS)
                def _():
                    pl.semaphore_wait(xfree.at[r], 1)

                for cp in xcopies(r, into, two, nxt):
                    cp.start()

            @pl.when((st >= 1) & (st <= 2 - link))
            def _():
                acc[r, slot] = part[...]

            @pl.when(st >= 3 - link)
            def _():
                acopy(slot, slot).wait_recv()
                acc[r, slot] += part[...]

            @pl.when((st == 1) & (link == 1))
            def _():
                send(acc, asend, arecv, r, 1, SLOTS, prv).start()

            @pl.when(st >= 1 + link)
            def _():
                @pl.when(st >= SLOTS)
                def _():
                    pl.semaphore_wait(afree.at[r], 1)

                acopy(slot, into).start()

        @pl.when(st == OWN_STEP)
        def _():
            tile(r, HOME)
            own[r] = part[...]

        @pl.when(i == n * RINGS + 2)
        def _():
            for cp in weight_grads():
                cp.start()

        @pl.when((st == n - 1) & (link == 0))
        def _():
            acopy(SLOTS, SLOTS).wait_recv()
            own[r] += acc[r, SLOTS]

        @pl.when(st == n)
        def _():
            acopy(slot, slot).wait_recv()
            own[r] += acc[r, slot]
            out[r] = own[r, 0:2 * t, :].astype(BF16)
            for cp in results(r):
                cp.start()

        return carry

    lax.fori_loop(0, (n + LAG + 1) * RINGS, step, 0)

    for cp in weight_grads():
        cp.wait()

    def end(r, carry):
        for cp in results(r):
            cp.wait()
        return carry

    lax.fori_loop(0, RINGS, end, 0)


def results_kernel(y_in, dx_in, dg_in, gw13_in, gw2_in, y_out, dx_out, dg_out, gw1_out, gw3_out, gw2_out,
                   y, dx, dg, gw13, gw2, in_sem, out_sem):
    el, ff, _ = gw2.shape
    bufs = (gw13, gw2, y, dx, dg)
    into = [pltpu.make_async_copy(a, b, in_sem.at[i]) for i, (a, b) in enumerate(zip((gw13_in, gw2_in, y_in, dx_in, dg_in), bufs))]
    for cp in into:
        cp.start()
    t = dg.shape[2]
    outs = []

    def put(src, dst):
        cp = pltpu.make_async_copy(src, dst, out_sem.at[len(outs)])
        cp.start()
        outs.append(cp)

    into[0].wait()
    for e in range(el):
        put(gw13.at[:, pl.ds(2 * e * ff, ff)], gw1_out.at[e])
        put(gw13.at[:, pl.ds((2 * e + 1) * ff, ff)], gw3_out.at[e])
    for cp, buf, dst in zip(into[1:4], bufs[1:4], (gw2_out, y_out, dx_out)):
        cp.wait()
        put(buf, dst)
    into[4].wait()
    for r in range(RINGS):
        put(dg.at[r], dg_out.at[:, pl.ds(r * t, t)])
    for cp in outs:
        cp.wait()


def solution(mesh):
    k = mesh.shape['row']
    n = k * mesh.shape['col']
    grp = ('row', 'col')
    tspec = P(('dp', 'row', 'col'), None)
    wspec = P(grp, None, None)
    gspec = P(('dp', 'row', 'col'), None, None)

    def local(x, ridx, gates, w1, w3, w2, dy):
        tok, d = x.shape
        top = ridx.shape[1]
        el, ff, _ = w2.shape
        t = tok // RINGS
        rows = 2 * t + top
        hbm = pl.BlockSpec(memory_space=pltpu.HBM)
        dma = pltpu.SemaphoreType.DMA((RINGS, SLOTS + 2))
        flops = 2 * n * tok * el * 9 * d * ff
        outs = pl.pallas_call(
            functools.partial(kernel, n, k),
            out_shape=(
                jax.ShapeDtypeStruct((tok, d), BF16),
                jax.ShapeDtypeStruct((tok, d), BF16),
                jax.ShapeDtypeStruct((RINGS, top, t), F32),
                jax.ShapeDtypeStruct((d, 2 * el * ff), F32),
                jax.ShapeDtypeStruct((el, ff, d), F32),
            ),
            in_specs=[hbm] * 7,
            out_specs=tuple([hbm] * 5),
            scratch_shapes=[
                pltpu.VMEM((RINGS, SLOTS + 2, rows, d), BF16),
                pltpu.VMEM((RINGS, SLOTS + 2, top, t), F32),
                pltpu.VMEM((RINGS, SLOTS + 1, rows, d), F32),
                pltpu.VMEM((RINGS, rows, d), F32),
                pltpu.VMEM((rows, d), F32),
                pltpu.VMEM((d, 2 * el * ff), F32),
                pltpu.VMEM((el, ff, d), F32),
                pltpu.VMEM((RINGS, 2 * t, d), BF16),
                pltpu.VMEM((top, tok), jnp.int32),
                pltpu.VMEM((d, el * ff), BF16),
                pltpu.VMEM((d, el * ff), BF16),
                pltpu.VMEM((el, ff, d), BF16),
                pltpu.VMEM((el, d, ff), BF16),
                pltpu.VMEM((el, 2 * ff, d), BF16),
                pltpu.SemaphoreType.DMA((RINGS + 3, max(3, el))),
                pltpu.SemaphoreType.DMA((RINGS + 1, 3)),
                dma, dma, dma, dma, dma, dma,
                pltpu.SemaphoreType.REGULAR((RINGS,)),
                pltpu.SemaphoreType.REGULAR((RINGS,)),
            ],
            compiler_params=pltpu.CompilerParams(
                collective_id=0, has_side_effects=True, vmem_limit_bytes=56 * 1024 * 1024),
            cost_estimate=pl.CostEstimate(flops=flops, bytes_accessed=4 * tok * d * 2, transcendentals=n * tok * el * ff),
            name='moe_ring',
        )(x, dy, gates.T, ridx.T, w1, w3, w2)
        y, dx, dg, gw1, gw3, gw2 = pl.pallas_call(
            results_kernel,
            out_shape=(
                jax.ShapeDtypeStruct((tok, d), BF16),
                jax.ShapeDtypeStruct((tok, d), BF16),
                jax.ShapeDtypeStruct((top, tok), F32),
                jax.ShapeDtypeStruct((el, d, ff), F32),
                jax.ShapeDtypeStruct((el, d, ff), F32),
                jax.ShapeDtypeStruct((el, ff, d), F32),
            ),
            in_specs=[hbm] * 5,
            out_specs=tuple([hbm] * 6),
            scratch_shapes=[pltpu.VMEM(o.shape, o.dtype) for o in outs] + [
                pltpu.SemaphoreType.DMA((5,)),
                pltpu.SemaphoreType.DMA((2 * el + 3 + RINGS,)),
            ],
            compiler_params=pltpu.CompilerParams(vmem_limit_bytes=56 * 1024 * 1024),
            name='moe_results',
        )(*outs)
        return y, dx, dg.T, gw1, gw3, gw2

    return jax.shard_map(local, mesh=mesh, in_specs=(tspec, tspec, tspec, wspec, wspec, wspec, tspec), out_specs=(tspec, tspec, tspec, gspec, gspec, gspec), check_vma=False)
```

```python
import functools

import jax
import jax.numpy as jnp
from jax import lax
from jax.experimental import pallas as pl
from jax.experimental.pallas import tpu as pltpu
from jax.sharding import PartitionSpec as P

RINGS = 4
SLOTS = 8
HOME = SLOTS + 1
LAG = 2
OWN_STEP = 5
MESH = pl.DeviceIdType.MESH
F32 = jnp.float32
BF16 = jnp.bfloat16


def dot(a, b):
    return jnp.dot(a, b, preferred_element_type=F32)


def tdot(a, b):
    return lax.dot_general(a, b, (((0,), (0,)), ((), ())), preferred_element_type=F32)


def neighbours(k):
    dp = lax.axis_index('dp')
    row = lax.axis_index('row')
    col = lax.axis_index('col')
    x = col // 2
    c = col % 2
    s = (row + x) % k
    last = (s + 1) // k
    first = 1 - (s + k - 1) // k
    b = 1 - c

    def at(r, q, core):
        return (dp, r % k, (q % k) * 2 + core)

    n1 = at(row + c * last, x + c * (1 - last), b)
    p1 = at(row + k - b * first, x + k - b * (1 - first), b)
    n2 = at(row + c * (1 - last), x + c * last, b)
    p2 = at(row + k - b * (1 - first), x + k - b * first, b)
    return (n1, p1), (n2, p2)


def pick(i, a, b):
    return tuple((1 - i) * p + i * q for p, q in zip(a, b))


def kernel(n, k, x_hbm, dy_hbm, g_hbm, id_hbm, w1_hbm, w3_hbm, w2_hbm,
           y_ref, dx_ref, dg_ref, gw13, gw2_ref,
           xs, gs, acc, own, part, ids, w1_ref, w3_ref, w2_ref, w2t_ref, w13t_ref,
           load_sem, xsend, xrecv, gsend, grecv, asend, arecv, xfree, afree):
    t = gs.shape[3]
    d = x_hbm.shape[1]
    el, ff, _ = w2_hbm.shape
    top = g_hbm.shape[0]
    h1, h2 = neighbours(k)
    core = lax.axis_index('col') % 2
    first_expert = (lax.axis_index('row') * lax.axis_size('col') + lax.axis_index('col')) * el

    barrier = pltpu.get_barrier_semaphore()
    for dev in (*h1, *h2):
        pl.semaphore_signal(barrier, inc=1, device_id=dev, device_id_type=MESH)

    def load(src, dst, i, j):
        cp = pltpu.make_async_copy(src, dst, load_sem.at[i, j])
        cp.start()
        return cp

    first = [load(id_hbm, ids, RINGS, 0)]
    for r in range(RINGS):
        rows = pl.ds(r * t, t)
        first.append(load(x_hbm.at[rows], xs.at[r, HOME, pl.ds(0, t)], r, 0))
        first.append(load(dy_hbm.at[rows], xs.at[r, HOME, pl.ds(t, t)], r, 1))
        first.append(load(g_hbm.at[:, rows], gs.at[r, HOME], r, 2))
    later = [load(w2_hbm, w2_ref, RINGS, 1)]
    for e in range(el):
        cols = pl.ds(e * ff, ff)
        later.append(load(w1_hbm.at[e], w1_ref.at[:, cols], RINGS + 1, e))
        later.append(load(w3_hbm.at[e], w3_ref.at[:, cols], RINGS + 2, e))

    for cp in first:
        cp.wait()
    for r in range(RINGS):
        xs[r, HOME, 2 * t:2 * t + top, :] = ids[:, r * t:(r + 1) * t].astype(F32).astype(BF16)
    gw13[...] = jnp.zeros_like(gw13)
    gw2_ref[...] = jnp.zeros_like(gw2_ref)
    pl.semaphore_wait(barrier, 4)

    def tile(r, slot):
        x = xs[r, slot, 0:t, :]
        dy = xs[r, slot, t:2 * t, :]
        gates = gs[r, slot, 0:top, :]
        dest = xs[r, slot, 2 * t:2 * t + top, :].astype(F32)
        hit = [dest == (first_expert + e).astype(F32) for e in range(el)]
        sub = lax.broadcasted_iota(jnp.int32, gates.shape, 0)
        rows = jnp.zeros_like(gates)
        for e in range(el):
            ge = jnp.sum(jnp.where(hit[e], gates, 0.0), axis=0, keepdims=True)
            me = jnp.max(jnp.where(hit[e], 1.0, 0.0), axis=0, keepdims=True)
            rows = jnp.where(sub == e, ge, jnp.where(sub == el + e, me, rows))
        colm = rows.T
        dyf = dy.astype(F32)
        ua = dot(x, w1_ref[...])
        va = dot(x, w3_ref[...])
        y = None
        dx = None
        dgc = jnp.zeros((t, 128), F32)
        lane = lax.broadcasted_iota(jnp.int32, dgc.shape, 1)
        dudv = []
        for e in range(el):
            g = colm[:, e:e + 1]
            m = colm[:, el + e:el + e + 1] > 0.5
            u = jnp.where(m, ua[:, e * ff:(e + 1) * ff].astype(BF16).astype(F32), 0.0)
            v = jnp.where(m, va[:, e * ff:(e + 1) * ff].astype(BF16).astype(F32), 0.0)
            s = jax.nn.sigmoid(u)
            us = u * s
            a = (us * v).astype(BF16)
            o = dot(a, w2_ref[e]).astype(BF16).astype(F32)
            yo = g * o
            y = yo if y is None else y + yo
            dgc = jnp.where(lane == e, jnp.sum(dyf * o, axis=1, keepdims=True), dgc)
            do = (g * dyf).astype(BF16)
            gw2_ref[e] += tdot(a, do)
            da = dot(do, w2t_ref[e])
            du = (da * v * s * (1.0 + u * (1.0 - s))).astype(BF16)
            dv = (da * us).astype(BF16)
            dd = jnp.concatenate([du, dv], axis=1)
            dudv.append(dd)
            de = dot(dd, w13t_ref[e]).astype(BF16).astype(F32)
            dx = de if dx is None else dx + de
        gw13[...] += tdot(x, jnp.concatenate(dudv, axis=1))
        part[0:t, :] = y
        part[t:2 * t, :] = dx
        dgr = dgc.T
        dg = jnp.zeros_like(gates)
        for e in range(el):
            dg = jnp.where(hit[e], dgr[e:e + 1, :], dg)
        part[2 * t:2 * t + top, :] = dg

    def ring(i):
        link = i // 2
        cyc = i % 2
        back = core + link * (1 - 2 * core)
        fwd = pick(cyc, h1[0], h2[0])
        bwd = pick(cyc, h1[1], h2[1])
        return link, 2 * cyc + back, pick(back, fwd, bwd), pick(back, bwd, fwd)

    def send(buf, sends, recvs, r, a, b, dev, s=None):
        return pltpu.make_async_remote_copy(
            src_ref=buf.at[r, a], dst_ref=buf.at[r, b], send_sem=sends.at[r, a if s is None else s],
            recv_sem=recvs.at[r, b], device_id=dev, device_id_type=MESH)

    def xcopies(r, a, b, dev, s=None):
        return send(gs, gsend, grecv, r, a, b, dev, s), send(xs, xsend, xrecv, r, a, b, dev, s)

    def begin(i, carry):
        link, r, nxt, prv = ring(RINGS - 1 - i)
        for cp in xcopies(r, HOME, 1, nxt):
            cp.start()

        @pl.when(link == 1)
        def _():
            for cp in xcopies(r, HOME, SLOTS, prv, SLOTS):
                cp.start()

        return carry

    lax.fori_loop(0, RINGS, begin, 0)

    for cp in later:
        cp.wait()
    for e in range(el):
        cols = slice(e * ff, (e + 1) * ff)
        w2t_ref[e] = w2_ref[e].astype(F32).T.astype(BF16)
        w13t_ref[e, 0:ff, :] = w1_ref[:, cols].astype(F32).T.astype(BF16)
        w13t_ref[e, ff:2 * ff, :] = w3_ref[:, cols].astype(F32).T.astype(BF16)

    def step(i, carry):
        link, r, nxt, prv = ring(i % RINGS)
        st = i // RINGS - 1 + link
        slot = (st + SLOTS) % SLOTS
        into = (st + 1) % SLOTS
        two = (st + 2) % SLOTS
        xslot = slot + (SLOTS - slot) * ((1 - link) * ((st + 1) // n))
        into_x = into + (SLOTS - into) * ((1 - link) * ((st + 2) // n))
        gone = (st + SLOTS - 1) % SLOTS
        done = st - LAG
        dslot = (st + 2 * SLOTS - LAG) % SLOTS

        def acopy(a, b):
            return send(acc, asend, arecv, r, a, b, nxt)

        @pl.when((st >= 2) & (st <= n - 1 - link))
        def _():
            for cp in xcopies(r, gone, gone, nxt):
                cp.wait_send()

        @pl.when(st == 2)
        def _():
            for cp in xcopies(r, HOME, HOME, nxt):
                cp.wait_send()

        @pl.when((st == 2) & (link == 1))
        def _():
            for cp in xcopies(r, HOME, SLOTS, prv, SLOTS):
                cp.wait_send()

        @pl.when((st >= 2) & (st <= n - 1 - SLOTS + link))
        def _():
            pl.semaphore_signal(xfree.at[r], inc=1, device_id=prv, device_id_type=MESH)

        @pl.when((done >= 1) & (done <= n - 1))
        def _():
            acopy(dslot, dslot).wait_send()

        @pl.when((done >= 1) & (done <= n - SLOTS))
        def _():
            pl.semaphore_signal(afree.at[r], inc=1, device_id=prv, device_id_type=MESH)

        @pl.when((st >= 0) & (st <= n - 1))
        def _():
            @pl.when(st >= 1)
            def _():
                tile(r, xslot)

            @pl.when(st <= n - 2)
            def _():
                for cp in xcopies(r, into_x, into_x, nxt):
                    cp.wait_recv()

            @pl.when(st <= n - 3 - link)
            def _():
                @pl.when(st + 2 > SLOTS)
                def _():
                    pl.semaphore_wait(xfree.at[r], 1)

                for cp in xcopies(r, into, two, nxt):
                    cp.start()

            @pl.when((st >= 1) & (st <= 2 - link))
            def _():
                acc[r, slot] = part[...]

            @pl.when(st >= 3 - link)
            def _():
                acopy(slot, slot).wait_recv()
                acc[r, slot] += part[...]

            @pl.when((st == 1) & (link == 1))
            def _():
                send(acc, asend, arecv, r, 1, SLOTS, prv).start()

            @pl.when(st >= 1 + link)
            def _():
                @pl.when(st >= SLOTS)
                def _():
                    pl.semaphore_wait(afree.at[r], 1)

                acopy(slot, into).start()

        @pl.when(st == OWN_STEP)
        def _():
            tile(r, HOME)
            own[r] = part[...]

        @pl.when((st == n - 1) & (link == 0))
        def _():
            acopy(SLOTS, SLOTS).wait_recv()
            own[r] += acc[r, SLOTS]

        @pl.when(st == n)
        def _():
            acopy(slot, slot).wait_recv()
            total = acc[r, slot] + own[r]
            rows = pl.ds(pl.multiple_of(r * t, t), t)
            y_ref[rows, :] = total[0:t].astype(BF16)
            dx_ref[rows, :] = total[t:2 * t].astype(BF16)
            dg_ref[r] = total[2 * t:2 * t + top]

        return carry

    lax.fori_loop(0, (n + LAG + 1) * RINGS, step, 0)


def results_kernel(y, dx, dg, gw13, gw2, y_out, dx_out, dg_out, gw1_out, gw3_out, gw2_out, sem):
    el, ff, _ = gw2.shape
    t = dg.shape[2]
    pairs = [(y, y_out), (dx, dx_out), (gw2, gw2_out)]
    for e in range(el):
        pairs.append((gw13.at[:, pl.ds(2 * e * ff, ff)], gw1_out.at[e]))
        pairs.append((gw13.at[:, pl.ds((2 * e + 1) * ff, ff)], gw3_out.at[e]))
    for r in range(RINGS):
        pairs.append((dg.at[r], dg_out.at[:, pl.ds(r * t, t)]))
    copies = [pltpu.make_async_copy(a, b, sem.at[i]) for i, (a, b) in enumerate(pairs)]
    for cp in copies:
        cp.start()
    for cp in copies:
        cp.wait()


def solution(mesh):
    k = mesh.shape['row']
    n = k * mesh.shape['col']
    grp = ('row', 'col')
    tspec = P(('dp', 'row', 'col'), None)
    wspec = P(grp, None, None)
    gspec = P(('dp', 'row', 'col'), None, None)

    def local(x, ridx, gates, w1, w3, w2, dy):
        tok, d = x.shape
        top = ridx.shape[1]
        el, ff, _ = w2.shape
        t = tok // RINGS
        rows = 2 * t + top
        vmem = pl.BlockSpec(memory_space=pltpu.VMEM)
        hbm = pl.BlockSpec(memory_space=pltpu.HBM)
        dma = pltpu.SemaphoreType.DMA((RINGS, SLOTS + 2))
        flops = 2 * n * tok * el * 9 * d * ff
        outs = pl.pallas_call(
            functools.partial(kernel, n, k),
            out_shape=(
                pltpu.VMEM((tok, d), BF16),
                pltpu.VMEM((tok, d), BF16),
                pltpu.VMEM((RINGS, top, t), F32),
                pltpu.VMEM((d, 2 * el * ff), F32),
                pltpu.VMEM((el, ff, d), F32),
            ),
            in_specs=[hbm] * 7,
            out_specs=tuple([vmem] * 5),
            scratch_shapes=[
                pltpu.VMEM((RINGS, SLOTS + 2, rows, d), BF16),
                pltpu.VMEM((RINGS, SLOTS + 2, top, t), F32),
                pltpu.VMEM((RINGS, SLOTS + 1, rows, d), F32),
                pltpu.VMEM((RINGS, rows, d), F32),
                pltpu.VMEM((rows, d), F32),
                pltpu.VMEM((top, tok), jnp.int32),
                pltpu.VMEM((d, el * ff), BF16),
                pltpu.VMEM((d, el * ff), BF16),
                pltpu.VMEM((el, ff, d), BF16),
                pltpu.VMEM((el, d, ff), BF16),
                pltpu.VMEM((el, 2 * ff, d), BF16),
                pltpu.SemaphoreType.DMA((RINGS + 3, max(3, el))),
                dma, dma, dma, dma, dma, dma,
                pltpu.SemaphoreType.REGULAR((RINGS,)),
                pltpu.SemaphoreType.REGULAR((RINGS,)),
            ],
            compiler_params=pltpu.CompilerParams(
                collective_id=0, has_side_effects=True, vmem_limit_bytes=48 * 1024 * 1024),
            cost_estimate=pl.CostEstimate(flops=flops, bytes_accessed=4 * tok * d * 2, transcendentals=n * tok * el * ff),
            name='moe_ring',
        )(*(pltpu.with_memory_space_constraint(a, pltpu.HBM) for a in (x, dy, gates.T, ridx.T, w1, w3, w2)))
        y, dx, dg, gw1, gw3, gw2 = pl.pallas_call(
            results_kernel,
            out_shape=(
                jax.ShapeDtypeStruct((tok, d), BF16),
                jax.ShapeDtypeStruct((tok, d), BF16),
                jax.ShapeDtypeStruct((top, tok), F32),
                jax.ShapeDtypeStruct((el, d, ff), F32),
                jax.ShapeDtypeStruct((el, d, ff), F32),
                jax.ShapeDtypeStruct((el, ff, d), F32),
            ),
            in_specs=[vmem] * 5,
            out_specs=tuple([hbm] * 6),
            scratch_shapes=[pltpu.SemaphoreType.DMA((2 * el + 3 + RINGS,))],
            compiler_params=pltpu.CompilerParams(vmem_limit_bytes=48 * 1024 * 1024),
            name='moe_results',
        )(*(pltpu.with_memory_space_constraint(a, pltpu.VMEM) for a in outs))
        return y, dx, dg.T, gw1, gw3, gw2

    return jax.shard_map(local, mesh=mesh, in_specs=(tspec, tspec, tspec, wspec, wspec, wspec, tspec), out_specs=(tspec, tspec, tspec, gspec, gspec, gspec), check_vma=False)
```

```python
import functools

import jax
import jax.numpy as jnp
from jax import lax
from jax.experimental import pallas as pl
from jax.experimental.pallas import tpu as pltpu
from jax.sharding import PartitionSpec as P

RINGS = 4
SLOTS = 8
HOME = SLOTS + 1
LAG = 2
OWN_STEP = 5
MESH = pl.DeviceIdType.MESH
F32 = jnp.float32
BF16 = jnp.bfloat16


def dot(a, b):
    return jnp.dot(a, b, preferred_element_type=F32)


def tdot(a, b):
    return lax.dot_general(a, b, (((0,), (0,)), ((), ())), preferred_element_type=F32)


def neighbours(k):
    dp = lax.axis_index('dp')
    row = lax.axis_index('row')
    col = lax.axis_index('col')
    x = col // 2
    c = col % 2
    s = (row + x) % k
    last = (s + 1) // k
    first = 1 - (s + k - 1) // k
    b = 1 - c

    def at(r, q, core):
        return (dp, r % k, (q % k) * 2 + core)

    n1 = at(row + c * last, x + c * (1 - last), b)
    p1 = at(row + k - b * first, x + k - b * (1 - first), b)
    n2 = at(row + c * (1 - last), x + c * last, b)
    p2 = at(row + k - b * (1 - first), x + k - b * first, b)
    return (n1, p1), (n2, p2)


def pick(i, a, b):
    return tuple((1 - i) * p + i * q for p, q in zip(a, b))


def kernel(n, k, x_hbm, dy_hbm, g_hbm, id_hbm, w1_hbm, w3_hbm, w2_hbm,
           y_ref, dx_ref, dg_ref, gw13, gw2_ref,
           xs, gs, acc, own, part, ids, w1_ref, w3_ref, w2_ref, w2t_ref, w13t_ref,
           load_sem, xsend, xrecv, gsend, grecv, asend, arecv, xfree, afree):
    t = gs.shape[3]
    d = x_hbm.shape[1]
    el, ff, _ = w2_hbm.shape
    top = g_hbm.shape[0]
    h1, h2 = neighbours(k)
    core = lax.axis_index('col') % 2
    first_expert = (lax.axis_index('row') * lax.axis_size('col') + lax.axis_index('col')) * el

    barrier = pltpu.get_barrier_semaphore()
    for dev in (*h1, *h2):
        pl.semaphore_signal(barrier, inc=1, device_id=dev, device_id_type=MESH)

    def load(src, dst, i, j):
        cp = pltpu.make_async_copy(src, dst, load_sem.at[i, j])
        cp.start()
        return cp

    first = [load(id_hbm, ids, RINGS, 0)]
    for r in range(RINGS):
        rows = pl.ds(r * t, t)
        first.append(load(x_hbm.at[rows], xs.at[r, HOME, pl.ds(0, t)], r, 0))
        first.append(load(dy_hbm.at[rows], xs.at[r, HOME, pl.ds(t, t)], r, 1))
        first.append(load(g_hbm.at[:, rows], gs.at[r, HOME], r, 2))
    later = [load(w2_hbm, w2_ref, RINGS, 1)]
    for e in range(el):
        cols = pl.ds(e * ff, ff)
        later.append(load(w1_hbm.at[e], w1_ref.at[:, cols], RINGS + 1, e))
        later.append(load(w3_hbm.at[e], w3_ref.at[:, cols], RINGS + 2, e))

    for cp in first:
        cp.wait()
    for r in range(RINGS):
        xs[r, HOME, 2 * t:2 * t + top, :] = ids[:, r * t:(r + 1) * t].astype(F32).astype(BF16)
    gw13[...] = jnp.zeros_like(gw13)
    gw2_ref[...] = jnp.zeros_like(gw2_ref)
    pl.semaphore_wait(barrier, 4)

    def tile(r, slot, gslot):
        x = xs[r, slot, 0:t, :]
        dy = xs[r, slot, t:2 * t, :]
        gates = gs[r, gslot]
        dest = xs[r, slot, 2 * t:2 * t + top, :].astype(F32)
        hit = [dest == (first_expert + e).astype(F32) for e in range(el)]
        sub = lax.broadcasted_iota(jnp.int32, gates.shape, 0)
        rows = jnp.zeros_like(gates)
        for e in range(el):
            ge = jnp.sum(jnp.where(hit[e], gates, 0.0), axis=0, keepdims=True)
            me = jnp.max(jnp.where(hit[e], 1.0, 0.0), axis=0, keepdims=True)
            rows = jnp.where(sub == e, ge, jnp.where(sub == el + e, me, rows))
        colm = rows.T
        dyf = dy.astype(F32)
        ua = dot(x, w1_ref[...])
        va = dot(x, w3_ref[...])
        y = None
        dx = None
        dgc = jnp.zeros((t, 128), F32)
        lane = lax.broadcasted_iota(jnp.int32, dgc.shape, 1)
        dudv = []
        for e in range(el):
            g = colm[:, e:e + 1]
            m = colm[:, el + e:el + e + 1] > 0.5
            u = jnp.where(m, ua[:, e * ff:(e + 1) * ff].astype(BF16).astype(F32), 0.0)
            v = jnp.where(m, va[:, e * ff:(e + 1) * ff].astype(BF16).astype(F32), 0.0)
            s = jax.nn.sigmoid(u)
            us = u * s
            a = (us * v).astype(BF16)
            o = dot(a, w2_ref[e]).astype(BF16).astype(F32)
            yo = g * o
            y = yo if y is None else y + yo
            dgc = jnp.where(lane == e, jnp.sum(dyf * o, axis=1, keepdims=True), dgc)
            do = (g * dyf).astype(BF16)
            gw2_ref[e] += tdot(a, do)
            da = dot(do, w2t_ref[e])
            du = (da * v * s * (1.0 + u * (1.0 - s))).astype(BF16)
            dv = (da * us).astype(BF16)
            dd = jnp.concatenate([du, dv], axis=1)
            dudv.append(dd)
            de = dot(dd, w13t_ref[e]).astype(BF16).astype(F32)
            dx = de if dx is None else dx + de
        gw13[...] += tdot(x, jnp.concatenate(dudv, axis=1))
        part[0:t, :] = y
        part[t:2 * t, :] = dx
        dgr = dgc.T
        for e in range(el):
            gates = jnp.where(hit[e], dgr[e:e + 1, :], gates)
        gs[r, gslot] = gates

    def ring(i):
        link = i // 2
        cyc = i % 2
        back = core + link * (1 - 2 * core)
        fwd = pick(cyc, h1[0], h2[0])
        bwd = pick(cyc, h1[1], h2[1])
        return link, 2 * cyc + back, pick(back, fwd, bwd), pick(back, bwd, fwd)

    def send(buf, sends, recvs, r, a, b, dev, s=None):
        return pltpu.make_async_remote_copy(
            src_ref=buf.at[r, a], dst_ref=buf.at[r, b], send_sem=sends.at[r, a if s is None else s],
            recv_sem=recvs.at[r, b], device_id=dev, device_id_type=MESH)

    def xcopy(r, a, b, dev, s=None):
        return send(xs, xsend, xrecv, r, a, b, dev, s)

    def begin(i, carry):
        link, r, nxt, prv = ring(RINGS - 1 - i)
        send(gs, gsend, grecv, r, HOME, 1, nxt).start()
        xcopy(r, HOME, 1, nxt).start()

        @pl.when(link == 1)
        def _():
            xcopy(r, HOME, SLOTS, prv, SLOTS).start()

        return carry

    lax.fori_loop(0, RINGS, begin, 0)

    for cp in later:
        cp.wait()
    for e in range(el):
        cols = slice(e * ff, (e + 1) * ff)
        w2t_ref[e] = w2_ref[e].astype(F32).T.astype(BF16)
        w13t_ref[e, 0:ff, :] = w1_ref[:, cols].astype(F32).T.astype(BF16)
        w13t_ref[e, ff:2 * ff, :] = w3_ref[:, cols].astype(F32).T.astype(BF16)

    def step(i, carry):
        link, r, nxt, prv = ring(i % RINGS)
        st = i // RINGS - 1 + link
        slot = (st + SLOTS) % SLOTS
        into = (st + 1) % SLOTS
        two = (st + 2) % SLOTS
        xslot = slot + (SLOTS - slot) * ((1 - link) * ((st + 1) // n))
        into_x = into + (SLOTS - into) * ((1 - link) * ((st + 2) // n))
        gone = (st + SLOTS - 1) % SLOTS
        done = st - LAG
        dslot = (st + 2 * SLOTS - LAG) % SLOTS

        def acopy(a, b):
            return send(acc, asend, arecv, r, a, b, nxt)

        def gcopy(a, b):
            return send(gs, gsend, grecv, r, a, b, nxt)

        @pl.when((st >= 2) & (st <= n - 1 - link))
        def _():
            xcopy(r, gone, gone, nxt).wait_send()

        @pl.when(st == 2)
        def _():
            gcopy(HOME, HOME).wait_send()
            xcopy(r, HOME, HOME, nxt).wait_send()

        @pl.when((st == 2) & (link == 1))
        def _():
            xcopy(r, HOME, SLOTS, prv, SLOTS).wait_send()

        @pl.when((st >= 2) & (st <= n - 1 - SLOTS + link))
        def _():
            pl.semaphore_signal(xfree.at[r], inc=1, device_id=prv, device_id_type=MESH)

        @pl.when((done >= 1) & (done <= n - 1))
        def _():
            gcopy(dslot, dslot).wait_send()
            acopy(dslot, dslot).wait_send()

        @pl.when((done >= 1) & (done <= n - SLOTS))
        def _():
            pl.semaphore_signal(afree.at[r], inc=1, device_id=prv, device_id_type=MESH)

        @pl.when((st >= 0) & (st <= n - 1))
        def _():
            @pl.when(st <= n - 2)
            def _():
                xcopy(r, into_x, into_x, nxt).wait_recv()

            @pl.when(st <= n - 3 - link)
            def _():
                @pl.when(st + 2 > SLOTS)
                def _():
                    pl.semaphore_wait(xfree.at[r], 1)

                xcopy(r, into, two, nxt).start()

            @pl.when(st >= 1)
            def _():
                gcopy(slot, slot).wait_recv()
                tile(r, xslot, slot)

                @pl.when(st >= SLOTS)
                def _():
                    pl.semaphore_wait(afree.at[r], 1)

                gcopy(slot, into).start()

            @pl.when((st >= 1) & (st <= 2 - link))
            def _():
                acc[r, slot] = part[...]

            @pl.when(st >= 3 - link)
            def _():
                acopy(slot, slot).wait_recv()
                acc[r, slot] += part[...]

            @pl.when((st == 1) & (link == 1))
            def _():
                send(acc, asend, arecv, r, 1, SLOTS, prv).start()

            @pl.when(st >= 1 + link)
            def _():
                acopy(slot, into).start()

        @pl.when(st == OWN_STEP)
        def _():
            tile(r, HOME, HOME)
            own[r] = part[...]

        @pl.when((st == n - 1) & (link == 0))
        def _():
            acopy(SLOTS, SLOTS).wait_recv()
            own[r] += acc[r, SLOTS]

        @pl.when(st == n)
        def _():
            gcopy(slot, slot).wait_recv()
            acopy(slot, slot).wait_recv()
            total = acc[r, slot] + own[r]
            rows = pl.ds(pl.multiple_of(r * t, t), t)
            y_ref[rows, :] = total[0:t].astype(BF16)
            dx_ref[rows, :] = total[t:2 * t].astype(BF16)
            mine = xs[r, HOME, 2 * t:2 * t + top, :].astype(F32) - first_expert.astype(F32)
            dg_ref[r] = jnp.where((mine >= 0.0) & (mine < el), gs[r, HOME], gs[r, slot])

        return carry

    lax.fori_loop(0, (n + LAG + 1) * RINGS, step, 0)


def results_kernel(y, dx, dg, gw13, gw2, y_out, dx_out, dg_out, gw1_out, gw3_out, gw2_out, sem):
    el, ff, _ = gw2.shape
    t = dg.shape[2]
    pairs = [(y, y_out), (dx, dx_out), (gw2, gw2_out)]
    for e in range(el):
        pairs.append((gw13.at[:, pl.ds(2 * e * ff, ff)], gw1_out.at[e]))
        pairs.append((gw13.at[:, pl.ds((2 * e + 1) * ff, ff)], gw3_out.at[e]))
    for r in range(RINGS):
        pairs.append((dg.at[r], dg_out.at[:, pl.ds(r * t, t)]))
    copies = [pltpu.make_async_copy(a, b, sem.at[i]) for i, (a, b) in enumerate(pairs)]
    for cp in copies:
        cp.start()
    for cp in copies:
        cp.wait()


def solution(mesh):
    k = mesh.shape['row']
    n = k * mesh.shape['col']
    grp = ('row', 'col')
    tspec = P(('dp', 'row', 'col'), None)
    wspec = P(grp, None, None)
    gspec = P(('dp', 'row', 'col'), None, None)

    def local(x, ridx, gates, w1, w3, w2, dy):
        tok, d = x.shape
        top = ridx.shape[1]
        el, ff, _ = w2.shape
        t = tok // RINGS
        rows = 2 * t + top
        vmem = pl.BlockSpec(memory_space=pltpu.VMEM)
        hbm = pl.BlockSpec(memory_space=pltpu.HBM)
        dma = pltpu.SemaphoreType.DMA((RINGS, SLOTS + 2))
        flops = 2 * n * tok * el * 9 * d * ff
        outs = pl.pallas_call(
            functools.partial(kernel, n, k),
            out_shape=(
                pltpu.VMEM((tok, d), BF16),
                pltpu.VMEM((tok, d), BF16),
                pltpu.VMEM((RINGS, top, t), F32),
                pltpu.VMEM((d, 2 * el * ff), F32),
                pltpu.VMEM((el, ff, d), F32),
            ),
            in_specs=[hbm] * 7,
            out_specs=tuple([vmem] * 5),
            scratch_shapes=[
                pltpu.VMEM((RINGS, SLOTS + 2, rows, d), BF16),
                pltpu.VMEM((RINGS, SLOTS + 2, top, t), F32),
                pltpu.VMEM((RINGS, SLOTS + 1, 2 * t, d), F32),
                pltpu.VMEM((RINGS, 2 * t, d), F32),
                pltpu.VMEM((2 * t, d), F32),
                pltpu.VMEM((top, tok), jnp.int32),
                pltpu.VMEM((d, el * ff), BF16),
                pltpu.VMEM((d, el * ff), BF16),
                pltpu.VMEM((el, ff, d), BF16),
                pltpu.VMEM((el, d, ff), BF16),
                pltpu.VMEM((el, 2 * ff, d), BF16),
                pltpu.SemaphoreType.DMA((RINGS + 3, max(3, el))),
                dma, dma, dma, dma, dma, dma,
                pltpu.SemaphoreType.REGULAR((RINGS,)),
                pltpu.SemaphoreType.REGULAR((RINGS,)),
            ],
            compiler_params=pltpu.CompilerParams(
                collective_id=0, has_side_effects=True, vmem_limit_bytes=48 * 1024 * 1024),
            cost_estimate=pl.CostEstimate(flops=flops, bytes_accessed=4 * tok * d * 2, transcendentals=n * tok * el * ff),
            name='moe_ring',
        )(*(pltpu.with_memory_space_constraint(a, pltpu.HBM) for a in (x, dy, gates.T, ridx.T, w1, w3, w2)))
        y, dx, dg, gw1, gw3, gw2 = pl.pallas_call(
            results_kernel,
            out_shape=(
                jax.ShapeDtypeStruct((tok, d), BF16),
                jax.ShapeDtypeStruct((tok, d), BF16),
                jax.ShapeDtypeStruct((top, tok), F32),
                jax.ShapeDtypeStruct((el, d, ff), F32),
                jax.ShapeDtypeStruct((el, d, ff), F32),
                jax.ShapeDtypeStruct((el, ff, d), F32),
            ),
            in_specs=[vmem] * 5,
            out_specs=tuple([hbm] * 6),
            scratch_shapes=[pltpu.SemaphoreType.DMA((2 * el + 3 + RINGS,))],
            compiler_params=pltpu.CompilerParams(vmem_limit_bytes=48 * 1024 * 1024),
            name='moe_results',
        )(*(pltpu.with_memory_space_constraint(a, pltpu.VMEM) for a in outs))
        return y, dx, dg.T, gw1, gw3, gw2

    return jax.shard_map(local, mesh=mesh, in_specs=(tspec, tspec, tspec, wspec, wspec, wspec, tspec), out_specs=(tspec, tspec, tspec, gspec, gspec, gspec), check_vma=False)
```

```python
import functools

import jax
import jax.numpy as jnp
from jax import lax
from jax.experimental import pallas as pl
from jax.experimental.pallas import tpu as pltpu
from jax.sharding import PartitionSpec as P

RINGS = 4
SLOTS = 8
HOME = SLOTS + 1
LAG = 2
OWN_STEP = 5
MESH = pl.DeviceIdType.MESH
F32 = jnp.float32
BF16 = jnp.bfloat16


def dot(a, b):
    return jnp.dot(a, b, preferred_element_type=F32)


def tdot(a, b):
    return lax.dot_general(a, b, (((0,), (0,)), ((), ())), preferred_element_type=F32)


def neighbours(k):
    dp = lax.axis_index('dp')
    row = lax.axis_index('row')
    col = lax.axis_index('col')
    x = col // 2
    c = col % 2
    s = (row + x) % k
    last = (s + 1) // k
    first = 1 - (s + k - 1) // k
    b = 1 - c

    def at(r, q, core):
        return (dp, r % k, (q % k) * 2 + core)

    n1 = at(row + c * last, x + c * (1 - last), b)
    p1 = at(row + k - b * first, x + k - b * (1 - first), b)
    n2 = at(row + c * (1 - last), x + c * last, b)
    p2 = at(row + k - b * (1 - first), x + k - b * first, b)
    return (n1, p1), (n2, p2)


def pick(i, a, b):
    return tuple((1 - i) * p + i * q for p, q in zip(a, b))


def kernel(n, k, x_hbm, dy_hbm, g_hbm, id_hbm, w1_hbm, w3_hbm, w2_hbm,
           y_ref, dx_ref, dg_ref, gw13, gw2_ref,
           xs, gs, acc, own, part, ids, w1_ref, w3_ref, w2_ref, w2t_ref, w13t_ref,
           load_sem, xsend, xrecv, gsend, grecv, asend, arecv, xfree, afree):
    t = gs.shape[3]
    d = x_hbm.shape[1]
    el, ff, _ = w2_hbm.shape
    top = g_hbm.shape[0]
    h1, h2 = neighbours(k)
    core = lax.axis_index('col') % 2
    first_expert = (lax.axis_index('row') * lax.axis_size('col') + lax.axis_index('col')) * el

    barrier = pltpu.get_barrier_semaphore()
    for dev in (*h1, *h2):
        pl.semaphore_signal(barrier, inc=1, device_id=dev, device_id_type=MESH)

    def load(src, dst, i, j):
        cp = pltpu.make_async_copy(src, dst, load_sem.at[i, j])
        cp.start()
        return cp

    first = [load(id_hbm, ids, RINGS, 0)]
    for r in range(RINGS):
        rows = pl.ds(r * t, t)
        first.append(load(x_hbm.at[rows], xs.at[r, HOME, pl.ds(0, t)], r, 0))
        first.append(load(dy_hbm.at[rows], xs.at[r, HOME, pl.ds(t, t)], r, 1))
        first.append(load(g_hbm.at[:, rows], gs.at[r, HOME], r, 2))
    later = [load(w2_hbm, w2_ref, RINGS, 1)]
    for e in range(el):
        cols = pl.ds(e * ff, ff)
        later.append(load(w1_hbm.at[e], w1_ref.at[:, cols], RINGS + 1, e))
        later.append(load(w3_hbm.at[e], w3_ref.at[:, cols], RINGS + 2, e))

    for cp in first:
        cp.wait()
    for r in range(RINGS):
        xs[r, HOME, 2 * t:2 * t + top, :] = ids[:, r * t:(r + 1) * t].astype(F32).astype(BF16)
    gw13[...] = jnp.zeros_like(gw13)
    gw2_ref[...] = jnp.zeros_like(gw2_ref)
    pl.semaphore_wait(barrier, 4)

    def tile(r, slot, gslot):
        x = xs[r, slot, 0:t, :]
        dy = xs[r, slot, t:2 * t, :]
        gates = gs[r, gslot]
        dest = xs[r, slot, 2 * t:2 * t + top, :].astype(F32)
        hit = [dest == (first_expert + e).astype(F32) for e in range(el)]
        sub = lax.broadcasted_iota(jnp.int32, gates.shape, 0)
        rows = jnp.zeros_like(gates)
        for e in range(el):
            ge = jnp.sum(jnp.where(hit[e], gates, 0.0), axis=0, keepdims=True)
            me = jnp.max(jnp.where(hit[e], 1.0, 0.0), axis=0, keepdims=True)
            rows = jnp.where(sub == e, ge, jnp.where(sub == el + e, me, rows))
        colm = rows.T
        dyf = dy.astype(F32)
        ua = dot(x, w1_ref[...])
        va = dot(x, w3_ref[...])
        y = None
        dx = None
        dgc = jnp.zeros((t, 128), F32)
        lane = lax.broadcasted_iota(jnp.int32, dgc.shape, 1)
        dudv = []
        for e in range(el):
            g = colm[:, e:e + 1]
            m = colm[:, el + e:el + e + 1] > 0.5
            u = jnp.where(m, ua[:, e * ff:(e + 1) * ff].astype(BF16).astype(F32), 0.0)
            v = jnp.where(m, va[:, e * ff:(e + 1) * ff].astype(BF16).astype(F32), 0.0)
            s = jax.nn.sigmoid(u)
            us = u * s
            a = (us * v).astype(BF16)
            o = dot(a, w2_ref[e]).astype(BF16).astype(F32)
            yo = g * o
            y = yo if y is None else y + yo
            dgc = jnp.where(lane == e, jnp.sum(dyf * o, axis=1, keepdims=True), dgc)
            do = (g * dyf).astype(BF16)
            gw2_ref[e] += tdot(a, do)
            da = dot(do, w2t_ref[e])
            du = (da * v * s * (1.0 + u * (1.0 - s))).astype(BF16)
            dv = (da * us).astype(BF16)
            dd = jnp.concatenate([du, dv], axis=1)
            dudv.append(dd)
            de = dot(dd, w13t_ref[e]).astype(BF16).astype(F32)
            dx = de if dx is None else dx + de
        gw13[...] += tdot(x, jnp.concatenate(dudv, axis=1))
        part[0:t, :] = y
        part[t:2 * t, :] = dx
        dgr = dgc.T
        for e in range(el):
            gates = jnp.where(hit[e], dgr[e:e + 1, :], gates)
        gs[r, gslot] = gates

    def ring(i):
        link = i % 2
        cyc = i // 2
        back = core + link * (1 - 2 * core)
        fwd = pick(cyc, h1[0], h2[0])
        bwd = pick(cyc, h1[1], h2[1])
        return link, 2 * cyc + back, pick(back, fwd, bwd), pick(back, bwd, fwd)

    def send(buf, sends, recvs, r, a, b, dev, s=None):
        return pltpu.make_async_remote_copy(
            src_ref=buf.at[r, a], dst_ref=buf.at[r, b], send_sem=sends.at[r, a if s is None else s],
            recv_sem=recvs.at[r, b], device_id=dev, device_id_type=MESH)

    def xcopy(r, a, b, dev, s=None):
        return send(xs, xsend, xrecv, r, a, b, dev, s)

    def begin(i, carry):
        link, r, nxt, prv = ring(RINGS - 1 - i)
        send(gs, gsend, grecv, r, HOME, 1, nxt).start()
        xcopy(r, HOME, 1, nxt).start()

        @pl.when(link == 1)
        def _():
            xcopy(r, HOME, SLOTS, prv, SLOTS).start()

        return carry

    lax.fori_loop(0, RINGS, begin, 0)

    for cp in later:
        cp.wait()
    for e in range(el):
        cols = slice(e * ff, (e + 1) * ff)
        w2t_ref[e] = w2_ref[e].astype(F32).T.astype(BF16)
        w13t_ref[e, 0:ff, :] = w1_ref[:, cols].astype(F32).T.astype(BF16)
        w13t_ref[e, ff:2 * ff, :] = w3_ref[:, cols].astype(F32).T.astype(BF16)

    def step(i, carry):
        link, r, nxt, prv = ring(i % RINGS)
        st = i // RINGS - 1 + link
        slot = (st + SLOTS) % SLOTS
        into = (st + 1) % SLOTS
        two = (st + 2) % SLOTS
        xslot = slot + (SLOTS - slot) * ((1 - link) * ((st + 1) // n))
        into_x = into + (SLOTS - into) * ((1 - link) * ((st + 2) // n))
        gone = (st + SLOTS - 1) % SLOTS
        done = st - LAG
        dslot = (st + 2 * SLOTS - LAG) % SLOTS

        def acopy(a, b):
            return send(acc, asend, arecv, r, a, b, nxt)

        def gcopy(a, b):
            return send(gs, gsend, grecv, r, a, b, nxt)

        @pl.when((st >= 2) & (st <= n - 1 - link))
        def _():
            xcopy(r, gone, gone, nxt).wait_send()

        @pl.when(st == 2)
        def _():
            gcopy(HOME, HOME).wait_send()
            xcopy(r, HOME, HOME, nxt).wait_send()

        @pl.when((st == 2) & (link == 1))
        def _():
            xcopy(r, HOME, SLOTS, prv, SLOTS).wait_send()

        @pl.when((st >= 2) & (st <= n - 1 - SLOTS + link))
        def _():
            pl.semaphore_signal(xfree.at[r], inc=1, device_id=prv, device_id_type=MESH)

        @pl.when((done >= 1) & (done <= n - 1))
        def _():
            gcopy(dslot, dslot).wait_send()
            acopy(dslot, dslot).wait_send()

        @pl.when((done >= 1) & (done <= n - SLOTS))
        def _():
            pl.semaphore_signal(afree.at[r], inc=1, device_id=prv, device_id_type=MESH)

        @pl.when((st >= 0) & (st <= n - 1))
        def _():
            @pl.when(st <= n - 2)
            def _():
                xcopy(r, into_x, into_x, nxt).wait_recv()

            @pl.when(st <= n - 3 - link)
            def _():
                @pl.when(st + 2 > SLOTS)
                def _():
                    pl.semaphore_wait(xfree.at[r], 1)

                xcopy(r, into, two, nxt).start()

            @pl.when(st >= 1)
            def _():
                gcopy(slot, slot).wait_recv()
                tile(r, xslot, slot)

                @pl.when(st >= SLOTS)
                def _():
                    pl.semaphore_wait(afree.at[r], 1)

                gcopy(slot, into).start()

            @pl.when((st >= 1) & (st <= 2 - link))
            def _():
                acc[r, slot] = part[...]

            @pl.when(st >= 3 - link)
            def _():
                acopy(slot, slot).wait_recv()
                acc[r, slot] += part[...]

            @pl.when((st == 1) & (link == 1))
            def _():
                send(acc, asend, arecv, r, 1, SLOTS, prv).start()

            @pl.when(st >= 1 + link)
            def _():
                acopy(slot, into).start()

        @pl.when(st == OWN_STEP)
        def _():
            tile(r, HOME, HOME)
            own[r] = part[...]

        @pl.when((st == n - 1) & (link == 0))
        def _():
            acopy(SLOTS, SLOTS).wait_recv()
            own[r] += acc[r, SLOTS]

        @pl.when(st == n)
        def _():
            gcopy(slot, slot).wait_recv()
            acopy(slot, slot).wait_recv()
            total = acc[r, slot] + own[r]
            rows = pl.ds(pl.multiple_of(r * t, t), t)
            y_ref[rows, :] = total[0:t].astype(BF16)
            dx_ref[rows, :] = total[t:2 * t].astype(BF16)
            mine = xs[r, HOME, 2 * t:2 * t + top, :].astype(F32) - first_expert.astype(F32)
            dg_ref[r] = jnp.where((mine >= 0.0) & (mine < el), gs[r, HOME], gs[r, slot])

        return carry

    lax.fori_loop(0, (n + LAG + 1) * RINGS, step, 0)


def results_kernel(y, dx, dg, gw13, gw2, y_out, dx_out, dg_out, gw1_out, gw3_out, gw2_out, sem):
    el, ff, _ = gw2.shape
    t = dg.shape[2]
    pairs = [(y, y_out), (dx, dx_out), (gw2, gw2_out)]
    for e in range(el):
        pairs.append((gw13.at[:, pl.ds(2 * e * ff, ff)], gw1_out.at[e]))
        pairs.append((gw13.at[:, pl.ds((2 * e + 1) * ff, ff)], gw3_out.at[e]))
    for r in range(RINGS):
        pairs.append((dg.at[r], dg_out.at[:, pl.ds(r * t, t)]))
    copies = [pltpu.make_async_copy(a, b, sem.at[i]) for i, (a, b) in enumerate(pairs)]
    for cp in copies:
        cp.start()
    for cp in copies:
        cp.wait()


def solution(mesh):
    k = mesh.shape['row']
    n = k * mesh.shape['col']
    grp = ('row', 'col')
    tspec = P(('dp', 'row', 'col'), None)
    wspec = P(grp, None, None)
    gspec = P(('dp', 'row', 'col'), None, None)

    def local(x, ridx, gates, w1, w3, w2, dy):
        tok, d = x.shape
        top = ridx.shape[1]
        el, ff, _ = w2.shape
        t = tok // RINGS
        rows = 2 * t + top
        vmem = pl.BlockSpec(memory_space=pltpu.VMEM)
        hbm = pl.BlockSpec(memory_space=pltpu.HBM)
        dma = pltpu.SemaphoreType.DMA((RINGS, SLOTS + 2))
        flops = 2 * n * tok * el * 9 * d * ff
        outs = pl.pallas_call(
            functools.partial(kernel, n, k),
            out_shape=(
                pltpu.VMEM((tok, d), BF16),
                pltpu.VMEM((tok, d), BF16),
                pltpu.VMEM((RINGS, top, t), F32),
                pltpu.VMEM((d, 2 * el * ff), F32),
                pltpu.VMEM((el, ff, d), F32),
            ),
            in_specs=[hbm] * 7,
            out_specs=tuple([vmem] * 5),
            scratch_shapes=[
                pltpu.VMEM((RINGS, SLOTS + 2, rows, d), BF16),
                pltpu.VMEM((RINGS, SLOTS + 2, top, t), F32),
                pltpu.VMEM((RINGS, SLOTS + 1, 2 * t, d), F32),
                pltpu.VMEM((RINGS, 2 * t, d), F32),
                pltpu.VMEM((2 * t, d), F32),
                pltpu.VMEM((top, tok), jnp.int32),
                pltpu.VMEM((d, el * ff), BF16),
                pltpu.VMEM((d, el * ff), BF16),
                pltpu.VMEM((el, ff, d), BF16),
                pltpu.VMEM((el, d, ff), BF16),
                pltpu.VMEM((el, 2 * ff, d), BF16),
                pltpu.SemaphoreType.DMA((RINGS + 3, max(3, el))),
                dma, dma, dma, dma, dma, dma,
                pltpu.SemaphoreType.REGULAR((RINGS,)),
                pltpu.SemaphoreType.REGULAR((RINGS,)),
            ],
            compiler_params=pltpu.CompilerParams(
                collective_id=0, has_side_effects=True, vmem_limit_bytes=48 * 1024 * 1024),
            cost_estimate=pl.CostEstimate(flops=flops, bytes_accessed=4 * tok * d * 2, transcendentals=n * tok * el * ff),
            name='moe_ring',
        )(*(pltpu.with_memory_space_constraint(a, pltpu.HBM) for a in (x, dy, gates.T, ridx.T, w1, w3, w2)))
        y, dx, dg, gw1, gw3, gw2 = pl.pallas_call(
            results_kernel,
            out_shape=(
                jax.ShapeDtypeStruct((tok, d), BF16),
                jax.ShapeDtypeStruct((tok, d), BF16),
                jax.ShapeDtypeStruct((top, tok), F32),
                jax.ShapeDtypeStruct((el, d, ff), F32),
                jax.ShapeDtypeStruct((el, d, ff), F32),
                jax.ShapeDtypeStruct((el, ff, d), F32),
            ),
            in_specs=[vmem] * 5,
            out_specs=tuple([hbm] * 6),
            scratch_shapes=[pltpu.SemaphoreType.DMA((2 * el + 3 + RINGS,))],
            compiler_params=pltpu.CompilerParams(vmem_limit_bytes=48 * 1024 * 1024),
            name='moe_results',
        )(*(pltpu.with_memory_space_constraint(a, pltpu.VMEM) for a in outs))
        return y, dx, dg.T, gw1, gw3, gw2

    return jax.shard_map(local, mesh=mesh, in_specs=(tspec, tspec, tspec, wspec, wspec, wspec, tspec), out_specs=(tspec, tspec, tspec, gspec, gspec, gspec), check_vma=False)
```
